32 devices in a mesh: pipe: 4 (over x, core), mp: 8 (over z, y).
Axes of the slice: x: 2, y: 2, z: 4, core: 2. Of those that a mesh axis runs over, the one named last changes fastest.
Arguments:
- hidden_in: bfloat16 [32, 8192], P(None, 'mp'), may hold values from -24000 to 24000
- lengths: int32 [32], replicated, may hold values from 1 to 256
- assign: int32 [32], replicated, may hold values from 0 to 31, each once
- token_ids: int32 [32], replicated, may hold values from 0 to 12287
- attn_gain: bfloat16 [4, 8192], P('pipe', 'mp'), may hold values from 0.099609375 to 1.8984375
- qkv_weight: bfloat16 [4, 8192, 5120], P('pipe', 'mp'), may hold values from -0.0625 to 0.0625
- qkv_bias: bfloat16 [4, 5120], P('pipe'), may hold values from -3 to 3
- out_weight: bfloat16 [4, 4096, 8192], P('pipe', None, 'mp'), may hold values from -0.375 to 0.375
- kv_cache: bfloat16 [4, 32, 2, 4, 256, 128], P('pipe', 'mp'), may hold values from -120 to 120
- final_gain: bfloat16 [8192], P('mp'), may hold values from 0.099609375 to 1.8984375
- head_weight: bfloat16 [8192, 12288], P(None, ('pipe', 'mp')), may hold values from -0.9923308 to 0.9923308
Outputs:
- logprobs: float32 [32, 12288], P(None, ('pipe', 'mp'))
- chosen: float32 [32], replicated
The draws below stay inside these ranges and needn't reach their ends.
Inputs may be any that keep to these rules, and one draw needn't show every extreme that they name: `assign`: a permutation of the 32 requests.
All inputs are finite; a program needn't handle non-finite values.
Results may differ from the reference program's by a relative error of at most 0.0017.
Values may be sent and summed in bfloat16 or wider, within the bound.
No kernel may reach another device: no remote copies, remote signals or barrier semaphores. Data moves between devices by JAX's collectives and lax.ppermute only.
A program may use at most 64 MiB of HBM per device.

```python
import math
import jax
import jax.numpy as jnp
import numpy as np
from jax import lax

D = 8192
HEADS = 32
KV_HEADS = 4
HEAD_DIM = 128
LEN = 256
LAYERS = 4
REQ = 32
QKV = 5120
VOCAB = 12288


def draw_kv_cache(key, part):
    base_draw = jnp.clip(jax.random.normal(jax.random.fold_in(key, 11), (LAYERS, REQ, 2, KV_HEADS, LEN, HEAD_DIM), jnp.float32), -4.0, 4.0)
    return base_draw.astype(jnp.bfloat16)


def column_profile(low_end, high_end):
    fraction = jnp.arange(D).astype(jnp.float32) / max(D - 1, 1)
    return low_end * jnp.exp(fraction * jnp.log(high_end / low_end))


def profiled_base(key):
    base_draw = jnp.clip(jax.random.normal(jax.random.fold_in(key, 21), (REQ, D), jnp.float32), -6.0, 6.0)
    profile = column_profile(3.0, 30.0)
    return base_draw * profile[None, :]


def draw_hidden_in(key, part):
    base_draw = profiled_base(key)
    return base_draw.astype(jnp.bfloat16)


def draw_head_weight(key, part):
    base_draw = jnp.clip(jax.random.normal(jax.random.fold_in(key, 24), (D, VOCAB), jnp.float32), -6.0, 6.0) * (3.0 * D ** (-0.5))
    return base_draw.astype(jnp.bfloat16)


def place_ends(drawn, rng, low, largest):
    place = [jax.random.randint(jax.random.fold_in(rng, axis), (), 0, length) for axis, length in enumerate(drawn.shape)]
    longest = drawn.shape.index(max(drawn.shape))
    neighbour = place[:longest] + [(place[longest] + 1) % drawn.shape[longest]] + place[longest + 1:]
    return drawn.at[tuple(place)].set(low).at[tuple(neighbour)].set(largest)


def block_scale(key, shape, pieces, least, high):
    def one(axis_at, parts):
        heights = jax.random.uniform(jax.random.fold_in(jax.random.fold_in(key, 6), axis_at), (parts,), jnp.float32, least / len(pieces), high / len(pieces))
        return jnp.repeat(jnp.exp(heights), shape[axis_at] // parts).reshape((-1,) + (1,) * (len(shape) - axis_at - 1))

    level = one(*pieces[0])
    for cut in pieces[1:]:
        level = level * one(*cut)
    return level


def rank_table(count, lean):
    portions = [(1 << 20) // math.isqrt(standing ** lean) + 1 for standing in range(1, count + 1)]
    scale = 1 + sum(portions) // (1 << 30)
    return np.cumsum(np.array([max(1, weight // scale) for weight in portions]))


def ranked_ids(own_key, extent, count, lean):
    table = rank_table(count, lean)
    ticket = jax.random.randint(jax.random.fold_in(own_key, 1), extent, 0, int(table[count - 1]))
    rank = jnp.searchsorted(jnp.asarray(table, jnp.int32), ticket, side="right")
    return jax.random.permutation(jax.random.fold_in(own_key, 2), count)[rank].astype(jnp.int32)


def bell_draw(own_key, shape, spread, bound, pieces=(), held_as=jnp.bfloat16):
    drawn = jax.random.normal(own_key, shape, jnp.float32) * spread
    if len(pieces) > 0:
        drawn = block_scale(own_key, shape, pieces, -0.22, 0.18) * drawn
    return jnp.clip(drawn, min=-bound, max=bound).astype(held_as)


def setup_inputs(seed: int = 0) -> dict:
    keys = jax.random.split(jax.random.key(seed), 12)
    return {
        "hidden_in": draw_hidden_in(jax.random.fold_in(keys[11], 71), 0),
        "lengths": place_ends(jax.random.randint(keys[1], (REQ,), 1, LEN + 1), jax.random.fold_in(keys[1], 1), 1, LEN).astype(jnp.int32),
        "assign": jax.random.permutation(keys[2], REQ).astype(jnp.int32),
        "token_ids": place_ends(ranked_ids(keys[3], (REQ,), VOCAB, 2), jax.random.fold_in(keys[3], 3), 0, VOCAB - 1).astype(jnp.int32),
        "attn_gain": jnp.clip(1.0 + 0.18 * jax.random.normal(keys[4], (LAYERS, D), jnp.float32), 0.099609375, 1.8984375).astype(jnp.bfloat16),
        "qkv_weight": bell_draw(keys[5], (LAYERS, D, QKV), D ** -0.5, 0.0625, ((0, 4), (1, 8))),
        "qkv_bias": bell_draw(keys[6], (LAYERS, QKV), 0.5, 3.0, ((0, 4),)),
        "out_weight": bell_draw(keys[7], (LAYERS, HEADS * HEAD_DIM, D), (HEADS * HEAD_DIM // 16) ** -0.5, 0.375, ((0, 4), (2, 8))),
        "kv_cache": draw_kv_cache(jax.random.fold_in(keys[11], 71), 0),
        "final_gain": jnp.clip(1.0 + 0.18 * jax.random.normal(keys[9], (D,), jnp.float32), 0.099609375, 1.8984375).astype(jnp.bfloat16),
        "head_weight": draw_head_weight(jax.random.fold_in(keys[11], 71), 0),
    }


EPS = 1e-06
THETA = 1000000.0

def rounded(values_in):
    return lax.optimization_barrier(values_in.astype(jnp.bfloat16)).astype(jnp.float32)

def rotate(values_in, positions):
    half_dim = values_in.shape[-1] // 2
    frequency = THETA ** (-jnp.arange(half_dim).astype(jnp.float32) * 2.0 / values_in.shape[-1])
    angles = positions.astype(jnp.float32)[:, None, None] * frequency[None, None, :]
    front_half = values_in[..., :half_dim]
    back_half = values_in[..., half_dim:]
    cosine = jnp.cos(angles)
    sine_part = jnp.sin(angles)
    return jnp.concatenate([front_half * cosine - back_half * sine_part, back_half * cosine + front_half * sine_part], axis=-1)

def reference(hidden_in, lengths, assign, token_ids, attn_gain, qkv_weight, qkv_bias, out_weight, kv_cache, final_gain, head_weight):
    stream = hidden_in[assign]
    positions = lengths[assign]
    group_size = HEADS // KV_HEADS
    query_cols = HEADS * HEAD_DIM
    key_cols = KV_HEADS * HEAD_DIM
    row_count = stream.shape[0]
    scale_factor = HEAD_DIM ** (-0.5)
    visible = jnp.arange(LEN).astype(jnp.int32)[None, :] < positions[:, None]
    key_mask = visible[:, None, None, :]
    for layer_index in range(LAYERS):
        current = stream.astype(jnp.float32)
        mean_sq = lax.optimization_barrier(jnp.mean(current * current, axis=1))
        scaled = (current * attn_gain[layer_index].astype(jnp.float32)).astype(jnp.bfloat16)
        projected = jnp.dot(scaled, qkv_weight[layer_index], preferred_element_type=jnp.float32)
        projected = projected * lax.rsqrt(mean_sq + EPS)[:, None] + qkv_bias[layer_index].astype(jnp.float32)
        queries = rotate(projected[:, :query_cols].reshape(row_count, HEADS, HEAD_DIM), positions).astype(jnp.bfloat16)
        key_new = rotate(projected[:, query_cols:query_cols + key_cols].reshape(row_count, KV_HEADS, HEAD_DIM), positions).astype(jnp.bfloat16)
        value_new = projected[:, query_cols + key_cols:].reshape(row_count, KV_HEADS, HEAD_DIM).astype(jnp.bfloat16)
        cache_rows = kv_cache[layer_index][assign].astype(jnp.float32)
        query_f = queries.astype(jnp.float32).reshape(row_count, KV_HEADS, group_size, HEAD_DIM)
        scores = jnp.einsum('rkgd,rkjd->rkgj', query_f, cache_rows[:, 0]) * scale_factor
        self_score = jnp.einsum('rkgd,rkd->rkg', query_f, key_new.astype(jnp.float32)) * scale_factor
        row_top = jnp.maximum(lax.optimization_barrier(jnp.max(jnp.where(key_mask, scores, -1e+30), axis=-1)), self_score)
        weights = jnp.where(key_mask, jnp.exp(scores - row_top[..., None]), 0.0)
        self_weight = jnp.exp(self_score - row_top)
        row_total = lax.optimization_barrier(jnp.sum(weights, axis=-1)) + self_weight
        summed = jnp.einsum('rkgj,rkjd->rkgd', rounded(weights), cache_rows[:, 1])
        summed = summed + rounded(self_weight)[..., None] * value_new.astype(jnp.float32)[:, :, None, :]
        attended = (summed / row_total[..., None]).astype(jnp.bfloat16).reshape(row_count, query_cols)
        update = jnp.dot(attended, out_weight[layer_index], preferred_element_type=jnp.float32)
        stream = (current + update).astype(jnp.bfloat16)
    current = stream.astype(jnp.float32)
    mean_sq = lax.optimization_barrier(jnp.mean(current * current, axis=1))
    normed = (current * final_gain.astype(jnp.float32) * lax.rsqrt(mean_sq + EPS)[:, None]).astype(jnp.bfloat16)
    logits = jnp.dot(normed, head_weight, preferred_element_type=jnp.float32)
    row_top = lax.optimization_barrier(jnp.max(logits, axis=1))
    row_total = lax.optimization_barrier(jnp.sum(jnp.exp(logits - row_top[:, None]), axis=1))
    logprobs = logits - (row_top + jnp.log(row_total))[:, None]
    targets = token_ids[assign]
    chosen = jnp.take_along_axis(logprobs, targets[:, None], axis=1)[:, 0]
    return (logprobs, chosen)
```

```python
import functools

import jax
import jax.numpy as jnp
from jax import lax
from jax.experimental import pallas as pl
from jax.experimental.pallas import tpu as pltpu
from jax.sharding import PartitionSpec as P

HEADS = 32
KV_HEADS = 4
HEAD_DIM = 128
GROUP = HEADS // KV_HEADS
EPS = 1e-06
THETA = 1000000.0
LANES = 128


def split_three(value):
    high = lax.reduce_precision(value, 8, 7)
    rest = value - high
    middle = lax.reduce_precision(rest, 8, 7)
    low = lax.reduce_precision(rest - middle, 8, 7)
    return high, middle, low


def attend_kernel(
    part_q, part_k, part_v, part_s, bias_q, bias_k, bias_v, cos_ref, sin_ref, upper_ref, cache_ref,
    out_ref, *, width,
):
    count = out_ref.shape[0]
    length = cache_ref.shape[3]
    squares = jnp.sum(jnp.sum(part_s[...].astype(jnp.float32), axis=0), axis=1, keepdims=True)
    inverse = lax.rsqrt(squares / width + EPS)
    cosine = cos_ref[...]
    sine = sin_ref[...]

    def project(part, bias):
        summed = jnp.sum(part[...].astype(jnp.float32), axis=0)
        return summed * inverse + bias[...].astype(jnp.float32)

    def rotate(head):
        return head * cosine + pltpu.roll(head, HEAD_DIM // 2, 1) * sine

    flat = project(part_q, bias_q)
    heads = [rotate(flat[:, g * HEAD_DIM : (g + 1) * HEAD_DIM]) for g in range(GROUP)]
    queries = jnp.concatenate(heads, axis=0).astype(jnp.bfloat16)
    key_new = rotate(project(part_k, bias_k)).astype(jnp.bfloat16).astype(jnp.float32)
    value_new = project(part_v, bias_v).astype(jnp.bfloat16).astype(jnp.float32)
    keys = cache_ref[:, 0, 0].reshape(count * length, HEAD_DIM)
    values = cache_ref[:, 1, 0].reshape(count * length, HEAD_DIM)
    scale = HEAD_DIM ** (-0.5)
    scores = (
        lax.dot_general(
            queries, keys, (((1,), (1,)), ((), ())), preferred_element_type=jnp.float32
        )
        * scale
    )
    tiled_key = jnp.concatenate([key_new] * GROUP, axis=0)
    tiled_value = jnp.concatenate([value_new] * GROUP, axis=0)
    self_score = (
        jnp.sum(queries.astype(jnp.float32) * tiled_key, axis=1, keepdims=True) * scale
    )
    rows = lax.broadcasted_iota(jnp.int32, scores.shape, 0) % count
    columns = lax.broadcasted_iota(jnp.int32, scores.shape, 1)
    visible = (columns >= rows * length) & (columns < upper_ref[...])
    top = jnp.maximum(jnp.max(jnp.where(visible, scores, -1e30), axis=1, keepdims=True), self_score)
    weights = jnp.where(visible, jnp.exp(scores - top), 0.0)
    self_weight = jnp.exp(self_score - top)
    total = jnp.sum(weights, axis=1, keepdims=True) + self_weight
    summed = jnp.dot(weights.astype(jnp.bfloat16), values, preferred_element_type=jnp.float32)
    summed = summed + self_weight.astype(jnp.bfloat16).astype(jnp.float32) * tiled_value
    attended = summed / total
    for g in range(GROUP):
        out_ref[:, g * HEAD_DIM : (g + 1) * HEAD_DIM] = attended[
            g * count : (g + 1) * count
        ].astype(jnp.bfloat16)


def attend(parts, bias, cosine, sine, upper, cache, width):
    peers, count, _ = parts.shape
    length = cache.shape[3]
    group_cols = GROUP * HEAD_DIM
    first_key = HEADS
    first_value = HEADS + KV_HEADS
    squares_at = HEADS + 2 * KV_HEADS
    head_part = lambda place: pl.BlockSpec((peers, count, HEAD_DIM), lambda k: (0, 0, place(k)))
    head_bias = lambda place: pl.BlockSpec((1, HEAD_DIM), lambda k: (0, place(k)))
    whole = lambda array: pl.BlockSpec(array.shape, lambda k: (0, 0))
    return pl.pallas_call(
        functools.partial(attend_kernel, width=width),
        grid=(KV_HEADS,),
        in_specs=[
            pl.BlockSpec((peers, count, group_cols), lambda k: (0, 0, k)),
            head_part(lambda k: first_key + k),
            head_part(lambda k: first_value + k),
            head_part(lambda k: squares_at),
            pl.BlockSpec((1, group_cols), lambda k: (0, k)),
            head_bias(lambda k: first_key + k),
            head_bias(lambda k: first_value + k),
            whole(cosine),
            whole(sine),
            whole(upper),
            pl.BlockSpec((count, 2, 1, length, HEAD_DIM), lambda k: (0, 0, k, 0, 0)),
        ],
        out_specs=pl.BlockSpec((count, group_cols), lambda k: (0, k)),
        out_shape=jax.ShapeDtypeStruct((count, HEADS * HEAD_DIM), jnp.bfloat16),
        name="attend",
    )(parts, parts, parts, parts, bias, bias, bias, cosine, sine, upper, cache)


def exchange(blocks, axis):
    return lax.all_to_all(blocks, axis, 0, 0, tiled=True)


def spread(value, axis):
    blocks = jnp.broadcast_to(value[None], (lax.axis_size(axis),) + value.shape)
    return exchange(blocks, axis)


def local(
    hidden_in,
    lengths,
    assign,
    token_ids,
    attn_gain,
    qkv_weight,
    qkv_bias,
    out_weight,
    kv_cache,
    final_gain,
    head_weight,
):
    sections = lax.axis_size("pipe")
    section = lax.axis_index("pipe")
    peers = lax.axis_size("mp")
    count = kv_cache.shape[1]
    length = kv_cache.shape[4]
    requests, share = hidden_in.shape
    width = share * peers
    first = lax.axis_index("mp") * count
    own_lengths = lax.dynamic_slice_in_dim(lengths, first, count, 0)
    half = HEAD_DIM // 2
    frequency = THETA ** (-jnp.arange(half).astype(jnp.float32) * 2.0 / HEAD_DIM)
    angles = own_lengths.astype(jnp.float32)[:, None] * frequency[None, :]
    cosine = jnp.cos(angles)
    sine = jnp.sin(angles)
    cosine = jnp.concatenate([cosine, cosine], axis=1)
    sine = jnp.concatenate([-sine, sine], axis=1)
    upper = jnp.arange(count, dtype=jnp.int32) * length + own_lengths
    upper = jnp.tile(upper, GROUP)[:, None]
    gain = attn_gain[0].astype(jnp.float32)
    weight_in = qkv_weight[0]
    weight_out = out_weight[0]
    cache = kv_cache[0]

    gain_blocks = jnp.broadcast_to(final_gain[None, None], (peers, 1, share))
    gain_full = lax.cond(section != 0, lambda b: exchange(b, "mp"), lambda b: b, gain_blocks)

    stream = hidden_in
    for layer in range(sections):
        active = section == layer
        current = stream.astype(jnp.float32)
        squares = jnp.sum(current * current, axis=1, keepdims=True)
        scaled = (current * gain).astype(jnp.bfloat16)
        partial_cols = jnp.dot(scaled, weight_in, preferred_element_type=jnp.float32)
        lane = lax.broadcasted_iota(jnp.int32, (requests, LANES), 1)
        high, middle, low = split_three(squares)
        tail = jnp.where(
            lane == 0, high, jnp.where(lane == 1, middle, jnp.where(lane == 2, low, 0.0))
        )
        payload = jnp.concatenate([partial_cols, tail], axis=1).astype(jnp.bfloat16)
        payload = payload.reshape(peers, count, -1)
        parts = lax.cond(active, lambda b: exchange(b, "mp"), lambda b: b, payload)
        attended = attend(parts, qkv_bias, cosine, sine, upper, cache, width)
        gathered = lax.cond(
            active,
            lambda b: spread(b, "mp"),
            lambda b: jnp.broadcast_to(b[None], (peers,) + b.shape),
            attended,
        )
        gathered = gathered.reshape(requests, -1)
        update = jnp.dot(gathered, weight_out, preferred_element_type=jnp.float32)
        stream = (current + update).astype(jnp.bfloat16)
        if layer + 1 < sections:
            stream = lax.ppermute(stream, "pipe", [(layer, layer + 1)])
        if layer == 0:
            gain_full, stream = lax.optimization_barrier((gain_full, stream))
            gain_full = lax.cond(section == 0, lambda b: exchange(b, "mp"), lambda b: b, gain_full)

    last = sections - 1
    odd = section % 2 == 1
    arrived = stream
    for target in range(1, last, 2):
        copied = lax.ppermute(stream, "pipe", [(last, target)])
        arrived = jnp.where(section == target, copied, arrived)
    rows = lax.cond(
        odd,
        lambda b: spread(b, "mp"),
        lambda b: jnp.broadcast_to(b[None], (peers,) + b.shape),
        arrived,
    )
    over = lax.ppermute(rows, "pipe", [(i, i - 1) for i in range(1, sections, 2)])
    rows = jnp.where(odd, rows, over)

    current = rows.astype(jnp.float32)
    squares = jnp.sum(current * current, axis=(0, 2))
    inverse = lax.rsqrt(squares / width + EPS)
    normed = (current * gain_full.astype(jnp.float32) * inverse[None, :, None]).astype(jnp.bfloat16)
    normed = jnp.transpose(normed, (1, 0, 2)).reshape(requests, width)
    placing = (assign[:, None] == jnp.arange(requests, dtype=jnp.int32)[None, :]).astype(
        jnp.bfloat16
    )
    normed = jnp.dot(placing, normed, preferred_element_type=jnp.float32).astype(jnp.bfloat16)
    logits = jnp.dot(normed, head_weight, preferred_element_type=jnp.float32)
    vocab = head_weight.shape[1]
    vocab_ids = lax.axis_index(("pipe", "mp")) * vocab + jnp.arange(vocab, dtype=jnp.int32)
    matches = vocab_ids[None, :] == token_ids[assign][:, None]
    picked = jnp.sum(jnp.where(matches, logits, 0.0), axis=1)
    local_top = jnp.max(logits, axis=1)
    local_total = jnp.sum(jnp.exp(logits - local_top[:, None]), axis=1)
    stats = spread(jnp.stack([local_top, local_total, picked]), ("pipe", "mp"))
    stats = stats.reshape(-1, 3, requests)
    row_top = jnp.max(stats[:, 0], axis=0)
    row_total = jnp.sum(stats[:, 1] * jnp.exp(stats[:, 0] - row_top[None, :]), axis=0)
    log_total = row_top + jnp.log(row_total)
    chosen = jnp.sum(stats[:, 2], axis=0) - log_total
    return (logits - log_total[:, None], chosen)


def solution(mesh):
    return jax.shard_map(
        local,
        mesh=mesh,
        in_specs=(
            P(None, "mp"),
            P(),
            P(),
            P(),
            P("pipe", "mp"),
            P("pipe", "mp", None),
            P("pipe", None),
            P("pipe", None, "mp"),
            P("pipe", "mp", None, None, None, None),
            P("mp"),
            P(None, ("pipe", "mp")),
        ),
        out_specs=(P(None, ("pipe", "mp")), P()),
        check_vma=False,
    )
```

```python
import functools

import jax
import jax.numpy as jnp
import numpy as np
from jax import lax
from jax.experimental import pallas as pl
from jax.experimental.pallas import tpu as pltpu
from jax.sharding import PartitionSpec as P

HEADS = 32
KV_HEADS = 4
HEAD_DIM = 128
GROUP = HEADS // KV_HEADS
EPS = 1e-06
THETA = 1000000.0
LANES = 128
CHUNK = 512
GRANT = 16 * 1024 * 1024

VMEM = pl.BlockSpec(memory_space=pltpu.VMEM)
SMEM = pl.BlockSpec(memory_space=pltpu.SMEM)
HBM = pl.BlockSpec(memory_space=pltpu.HBM)
PARAMS = pltpu.CompilerParams(vmem_limit_bytes=GRANT)


def in_hbm(array):
    return pltpu.with_memory_space_constraint(array, pltpu.HBM)


def in_vmem(array):
    return pltpu.with_memory_space_constraint(array, pltpu.VMEM)


def column_copies(source, target, sem):
    return [
        pltpu.make_async_copy(
            source.at[:, pl.ds(i * CHUNK, CHUNK)], target.at[:, pl.ds(i * CHUNK, CHUNK)], sem.at[i]
        )
        for i in range(target.shape[1] // CHUNK)
    ]


def project_body(stream_ref, gain_ref, weight, out_ref, copies):
    peers, count, _ = out_ref.shape
    current = stream_ref[...].astype(jnp.float32)
    squares = jnp.sum(current * current, axis=1, keepdims=True)
    scaled = (current * gain_ref[...].astype(jnp.float32)).astype(jnp.bfloat16)
    high = squares.astype(jnp.bfloat16).astype(jnp.float32)
    middle = (squares - high).astype(jnp.bfloat16).astype(jnp.float32)
    low = squares - high - middle
    lane = lax.broadcasted_iota(jnp.int32, (current.shape[0], LANES), 1)
    tail = jnp.where(lane == 0, high, jnp.where(lane == 1, middle, jnp.where(lane == 2, low, 0.0)))

    def store(block, at):
        for j in range(peers):
            out_ref[j, :, at : at + block.shape[1]] = block[j * count : (j + 1) * count].astype(
                jnp.bfloat16
            )

    store(tail, weight.shape[1])
    for i in range(weight.shape[1] // CHUNK):
        if copies is not None:
            copies[i].wait()
        block = jnp.dot(
            scaled,
            weight[:, i * CHUNK : (i + 1) * CHUNK],
            preferred_element_type=jnp.float32,
        )
        store(block, i * CHUNK)


def project_first_kernel(stream_ref, gain_ref, source_ref, out_ref, weight_ref, sem):
    copies = column_copies(source_ref, weight_ref, sem)
    for copy in copies:
        copy.start()
    project_body(stream_ref, gain_ref, weight_ref, out_ref, copies)


def project_kernel(stream_ref, gain_ref, weight_ref, out_ref):
    project_body(stream_ref, gain_ref, weight_ref, out_ref, None)


def project_first(stream, gain, weight, peers):
    columns = weight.shape[1]
    count = stream.shape[0] // peers
    return pl.pallas_call(
        project_first_kernel,
        in_specs=[VMEM, VMEM, HBM],
        out_specs=[VMEM, VMEM],
        out_shape=[
            jax.ShapeDtypeStruct((peers, count, columns + LANES), jnp.bfloat16),
            pltpu.VMEM(weight.shape, weight.dtype),
        ],
        scratch_shapes=[pltpu.SemaphoreType.DMA((columns // CHUNK,))],
        compiler_params=PARAMS,
        name="project_first",
    )(stream, gain, in_hbm(weight))


def project(stream, gain, weight, peers):
    columns = weight.shape[1]
    count = stream.shape[0] // peers
    return pl.pallas_call(
        project_kernel,
        in_specs=[VMEM, VMEM, VMEM],
        out_specs=VMEM,
        out_shape=jax.ShapeDtypeStruct((peers, count, columns + LANES), jnp.bfloat16),
        compiler_params=PARAMS,
        name="project",
    )(stream, gain, in_vmem(weight))


def attend_body(lengths_ref, place_ref, parts_ref, bias_ref, frequency_ref, cache, out_ref, width, ready):
    count = out_ref.shape[0]
    length = cache.shape[3]
    query_cols = HEADS * HEAD_DIM
    key_cols = KV_HEADS * HEAD_DIM
    first = place_ref[0] * count
    at_row = lax.broadcasted_iota(jnp.int32, (count, HEAD_DIM), 0)
    positions = jnp.zeros((count, HEAD_DIM), jnp.int32)
    wide = (GROUP * count, count * length)
    rows = lax.broadcasted_iota(jnp.int32, wide, 0) % count
    columns = lax.broadcasted_iota(jnp.int32, wide, 1)
    visible = columns < 0
    for r in range(count):
        position = lengths_ref[first + r]
        positions = jnp.where(at_row == r, position, positions)
        mine = (rows == r) & (columns >= r * length) & (columns < r * length + position)
        visible = visible | mine
    angles = positions.astype(jnp.float32) * frequency_ref[...]
    lane = lax.broadcasted_iota(jnp.int32, (count, HEAD_DIM), 1)
    cosine = jnp.cos(angles)
    sine = jnp.sin(angles)
    sine = jnp.where(lane < HEAD_DIM // 2, -sine, sine)

    def total_of(at, size):
        acc = parts_ref[0, :, at : at + size].astype(jnp.float32)
        for j in range(1, parts_ref.shape[0]):
            acc = acc + parts_ref[j, :, at : at + size].astype(jnp.float32)
        return acc

    squares = jnp.sum(total_of(query_cols + 2 * key_cols, LANES), axis=1, keepdims=True)
    inverse = lax.rsqrt(squares / width + EPS)

    def columns_of(at):
        bias = bias_ref[:, at : at + HEAD_DIM].astype(jnp.float32)
        return total_of(at, HEAD_DIM) * inverse + bias

    def rotate(head):
        return head * cosine + pltpu.roll(head, HEAD_DIM // 2, 1) * sine

    scale = HEAD_DIM ** (-0.5)
    heads = []
    for k in range(KV_HEADS):
        stack = [rotate(columns_of((k * GROUP + g) * HEAD_DIM)) for g in range(GROUP)]
        queries = jnp.concatenate(stack, axis=0).astype(jnp.bfloat16)
        key_new = rotate(columns_of(query_cols + k * HEAD_DIM))
        key_new = key_new.astype(jnp.bfloat16).astype(jnp.float32)
        value_new = columns_of(query_cols + key_cols + k * HEAD_DIM)
        value_new = value_new.astype(jnp.bfloat16).astype(jnp.float32)
        heads.append((queries, key_new, value_new))
    ready()
    for k in range(KV_HEADS):
        queries, key_new, value_new = heads[k]
        keys = cache[:, 0, k].reshape(count * length, HEAD_DIM)
        values = cache[:, 1, k].reshape(count * length, HEAD_DIM)
        scores = (
            lax.dot_general(
                queries, keys, (((1,), (1,)), ((), ())), preferred_element_type=jnp.float32
            )
            * scale
        )
        tiled_key = jnp.concatenate([key_new] * GROUP, axis=0)
        tiled_value = jnp.concatenate([value_new] * GROUP, axis=0)
        self_score = (
            jnp.sum(queries.astype(jnp.float32) * tiled_key, axis=1, keepdims=True) * scale
        )
        top = jnp.max(jnp.where(visible, scores, -1e30), axis=1, keepdims=True)
        top = jnp.maximum(top, self_score)
        weights = jnp.where(visible, jnp.exp(scores - top), 0.0)
        self_weight = jnp.exp(self_score - top)
        total = jnp.sum(weights, axis=1, keepdims=True) + self_weight
        summed = jnp.dot(weights.astype(jnp.bfloat16), values, preferred_element_type=jnp.float32)
        summed = summed + self_weight.astype(jnp.bfloat16).astype(jnp.float32) * tiled_value
        attended = summed / total
        for g in range(GROUP):
            at = (k * GROUP + g) * HEAD_DIM
            out_ref[:, at : at + HEAD_DIM] = attended[g * count : (g + 1) * count].astype(
                jnp.bfloat16
            )


def attend_first_kernel(
    lengths_ref, place_ref, parts_ref, bias_ref, frequency_ref, cache_hbm, weight_hbm,
    out_ref, cache_ref, weight_ref, sem, *, width,
):
    copy_cache = pltpu.make_async_copy(cache_hbm, cache_ref, sem.at[0])
    copy_weight = pltpu.make_async_copy(weight_hbm, weight_ref, sem.at[1])
    copy_cache.start()
    copy_weight.start()
    attend_body(
        lengths_ref, place_ref, parts_ref, bias_ref, frequency_ref, cache_ref, out_ref, width,
        copy_cache.wait,
    )
    copy_weight.wait()


def attend_kernel(
    lengths_ref, place_ref, parts_ref, bias_ref, frequency_ref, cache_ref, out_ref, *, width
):
    attend_body(
        lengths_ref, place_ref, parts_ref, bias_ref, frequency_ref, cache_ref, out_ref, width,
        lambda: None,
    )


def attend_first(lengths, place, parts, bias, frequency, cache, weight, width):
    count = parts.shape[1]
    return pl.pallas_call(
        functools.partial(attend_first_kernel, width=width),
        in_specs=[SMEM, SMEM, VMEM, VMEM, VMEM, HBM, HBM],
        out_specs=[VMEM, VMEM, VMEM],
        out_shape=[
            jax.ShapeDtypeStruct((count, HEADS * HEAD_DIM), jnp.bfloat16),
            pltpu.VMEM(cache.shape, cache.dtype),
            pltpu.VMEM(weight.shape, weight.dtype),
        ],
        scratch_shapes=[pltpu.SemaphoreType.DMA((2,))],
        compiler_params=PARAMS,
        name="attend_first",
    )(lengths, place, parts, bias, frequency, in_hbm(cache), in_hbm(weight))


def attend(lengths, place, parts, bias, frequency, cache, width):
    count = parts.shape[1]
    return pl.pallas_call(
        functools.partial(attend_kernel, width=width),
        in_specs=[SMEM, SMEM, VMEM, VMEM, VMEM, VMEM],
        out_specs=VMEM,
        out_shape=jax.ShapeDtypeStruct((count, HEADS * HEAD_DIM), jnp.bfloat16),
        compiler_params=PARAMS,
        name="attend",
    )(lengths, place, parts, bias, frequency, in_vmem(cache))


def combine_kernel(gathered_ref, weight_ref, stream_ref, out_ref):
    peers = gathered_ref.shape[0]
    blocks = [gathered_ref[j].astype(jnp.float32) for j in range(peers)]
    gathered = jnp.concatenate(blocks, axis=0).astype(jnp.bfloat16)
    for at in range(0, out_ref.shape[1], 256):
        update = jnp.dot(
            gathered, weight_ref[:, at : at + 256], preferred_element_type=jnp.float32
        )
        current = stream_ref[:, at : at + 256].astype(jnp.float32)
        out_ref[:, at : at + 256] = (current + update).astype(jnp.bfloat16)


def combine(gathered, weight, stream):
    return pl.pallas_call(
        combine_kernel,
        in_specs=[VMEM, VMEM, VMEM],
        out_specs=VMEM,
        out_shape=jax.ShapeDtypeStruct(stream.shape, jnp.bfloat16),
        compiler_params=PARAMS,
        name="combine",
    )(gathered, in_vmem(weight), stream)


def load_kernel(idle_ref, source_ref, out_ref, sem):
    @pl.when(idle_ref[0] == 1)
    def _():
        copy = pltpu.make_async_copy(source_ref, out_ref, sem.at[0])
        copy.start()
        copy.wait()


def load_rest_kernel(idle_ref, source_ref, before_ref, out_ref, sem):
    del before_ref
    load_kernel(idle_ref, source_ref, out_ref, sem)


def load(idle, weight, before=None):
    first = before is None
    return pl.pallas_call(
        load_kernel if first else load_rest_kernel,
        in_specs=[SMEM, HBM] + ([] if first else [VMEM]),
        out_specs=VMEM,
        out_shape=pltpu.VMEM(weight.shape, weight.dtype),
        scratch_shapes=[pltpu.SemaphoreType.DMA((1,))],
        compiler_params=PARAMS,
        input_output_aliases={} if first else {2: 0},
        name="load" if first else "load_rest",
    )(idle, in_hbm(weight), *([] if first else [in_vmem(before)]))


def logits_kernel(
    assign_ref, tokens_ref, place_ref, rows_ref, over_ref, gain_ref, weight_ref,
    logits_ref, stats_ref, scratch_ref, *, width,
):
    pieces, requests, share = rows_ref.shape
    vocab = weight_ref.shape[1]
    own = place_ref[1] == 1
    squares = jnp.zeros((requests, 1), jnp.float32)
    for m in range(pieces):
        current = jnp.where(own, rows_ref[m], over_ref[m]).astype(jnp.float32)
        squares = squares + jnp.sum(current * current, axis=1, keepdims=True)
    inverse = lax.rsqrt(squares / width + EPS)
    logits = jnp.zeros((requests, vocab), jnp.float32)
    for m in range(pieces):
        current = jnp.where(own, rows_ref[m], over_ref[m]).astype(jnp.float32)
        normed = (current * gain_ref[m].astype(jnp.float32) * inverse).astype(jnp.bfloat16)
        logits = logits + jnp.dot(
            normed, weight_ref[m * share : (m + 1) * share], preferred_element_type=jnp.float32
        )
    scratch_ref[...] = logits
    row = lax.broadcasted_iota(jnp.int32, (requests, vocab), 0)
    targets = jnp.zeros((requests, vocab), jnp.int32)
    for s in range(requests):
        request = assign_ref[s]
        logits_ref[pl.ds(s, 1), :] = scratch_ref[pl.ds(request, 1), :]
        targets = jnp.where(row == s, tokens_ref[request] - place_ref[0], targets)
    ordered = logits_ref[...]
    column = lax.broadcasted_iota(jnp.int32, (requests, vocab), 1)
    picked = jnp.sum(jnp.where(column == targets, ordered, 0.0), axis=1, keepdims=True)
    top = jnp.max(ordered, axis=1, keepdims=True)
    total = jnp.sum(jnp.exp(ordered - top), axis=1, keepdims=True)
    wide = (requests, stats_ref.shape[1])
    lane = lax.broadcasted_iota(jnp.int32, wide, 1) - lax.broadcasted_iota(jnp.int32, wide, 0)
    spread_out = jnp.where(lane == 0, top, 0.0)
    spread_out = jnp.where(lane == requests, total, spread_out)
    spread_out = jnp.where(lane == 2 * requests, picked, spread_out)
    stats_ref[...] = jnp.sum(spread_out, axis=0, keepdims=True)


def final_logits(assign, tokens, place, rows, over, gain, weight, width):
    requests = rows.shape[1]
    vocab = weight.shape[1]
    lanes = -(-3 * requests // LANES) * LANES
    return pl.pallas_call(
        functools.partial(logits_kernel, width=width),
        in_specs=[SMEM, SMEM, SMEM, VMEM, VMEM, VMEM, VMEM],
        out_specs=[VMEM, VMEM],
        out_shape=[
            jax.ShapeDtypeStruct((requests, vocab), jnp.float32),
            jax.ShapeDtypeStruct((1, lanes), jnp.float32),
        ],
        scratch_shapes=[pltpu.VMEM((requests, vocab), jnp.float32)],
        compiler_params=PARAMS,
        name="final_logits",
    )(assign, tokens, place, rows, over, gain, in_vmem(weight))


def finish_kernel(logits_ref, stats_ref, out_ref, chosen_ref):
    requests = logits_ref.shape[0]
    stats = stats_ref[...]
    lanes = stats.shape[1]
    top = jnp.max(stats, axis=0, keepdims=True)
    sums = pltpu.roll(stats, lanes - requests, 1)
    picks = pltpu.roll(stats, lanes - 2 * requests, 1)
    total = jnp.sum(sums * jnp.exp(jnp.minimum(stats - top, 0.0)), axis=0, keepdims=True)
    lane = lax.broadcasted_iota(jnp.int32, (1, lanes), 1)
    total = jnp.where(lane < requests, total, 1.0)
    log_total = jnp.where(lane < requests, top, 0.0) + jnp.log(total)
    chosen_ref[...] = (jnp.sum(picks, axis=0, keepdims=True) - log_total)[:, :requests]
    wide = (requests, lanes)
    here = lax.broadcasted_iota(jnp.int32, wide, 1) == lax.broadcasted_iota(jnp.int32, wide, 0)
    column = jnp.sum(jnp.where(here, log_total, 0.0), axis=1, keepdims=True)
    out_ref[...] = logits_ref[...] - column


def finish(logits, stats):
    requests = logits.shape[0]
    return pl.pallas_call(
        finish_kernel,
        in_specs=[VMEM, VMEM],
        out_specs=[VMEM, VMEM],
        out_shape=[
            jax.ShapeDtypeStruct(logits.shape, jnp.float32),
            jax.ShapeDtypeStruct((1, requests), jnp.float32),
        ],
        compiler_params=PARAMS,
        name="finish",
    )(logits, stats)


def exchange(blocks, axis):
    return lax.all_to_all(blocks, axis, 0, 0, tiled=True)


def spread(value, axis):
    blocks = jnp.broadcast_to(value[None], (lax.axis_size(axis),) + value.shape)
    return exchange(blocks, axis)


def local(
    hidden_in,
    lengths,
    assign,
    token_ids,
    attn_gain,
    qkv_weight,
    qkv_bias,
    out_weight,
    kv_cache,
    final_gain,
    head_weight,
):
    sections = lax.axis_size("pipe")
    section = lax.axis_index("pipe")
    peers = lax.axis_size("mp")
    share = hidden_in.shape[1]
    width = share * peers
    place = lax.axis_index("mp").astype(jnp.int32).reshape(1)
    exponents = np.arange(HEAD_DIM // 2, dtype=np.float64) * 2.0 / HEAD_DIM
    frequency = np.tile(THETA ** (-exponents), 2)[None, :].astype(np.float32)
    weight_in = qkv_weight[0]
    weight_out = out_weight[0]
    cache = kv_cache[0]

    gain_blocks = jnp.broadcast_to(final_gain[None, None], (peers, 1, share))
    gain_full = lax.cond(section != 0, lambda b: exchange(b, "mp"), lambda b: b, gain_blocks)

    def only_active(active, fn, other, value):
        return lax.cond(active, fn, other, value)

    stream = hidden_in
    for layer in range(sections):
        active = section == layer
        if layer == 0:
            payload, weight_in = project_first(stream, attn_gain, weight_in, peers)
        else:
            payload = project(stream, attn_gain, weight_in, peers)
        parts = lax.cond(active, lambda b: exchange(b, "mp"), lambda b: b, payload)
        if layer == 0:
            attended, cache, weight_out = attend_first(
                lengths, place, parts, qkv_bias, frequency, cache, weight_out, width
            )
        else:
            attended = attend(lengths, place, parts, qkv_bias, frequency, cache, width)
        gathered = lax.cond(
            active,
            lambda b: spread(b, "mp"),
            lambda b: jnp.broadcast_to(b[None], (peers,) + b.shape),
            attended,
        )
        stream = combine(gathered, weight_out, stream)
        if layer + 1 < sections:
            stream = lax.ppermute(stream, "pipe", [(layer, layer + 1)])
        if layer == 0:
            gain_full, stream = lax.optimization_barrier((gain_full, stream))
            gain_full = lax.cond(section == 0, lambda b: exchange(b, "mp"), lambda b: b, gain_full)
            weight_head = load((section != 0).astype(jnp.int32).reshape(1), head_weight)
        if layer == 1:
            weight_head = load((section == 0).astype(jnp.int32).reshape(1), head_weight, weight_head)

    last = sections - 1
    odd = section % 2 == 1
    arrived = stream
    for target in range(1, last, 2):
        copied = lax.ppermute(stream, "pipe", [(last, target)])
        arrived = jnp.where(section == target, copied, arrived)
    rows = lax.cond(
        odd,
        lambda b: spread(b, "mp"),
        lambda b: jnp.broadcast_to(b[None], (peers,) + b.shape),
        arrived,
    )
    over = lax.ppermute(rows, "pipe", [(i, i - 1) for i in range(1, sections, 2)])

    vocab_first = lax.axis_index(("pipe", "mp")) * head_weight.shape[1]
    head_place = jnp.stack([vocab_first, odd.astype(vocab_first.dtype)]).astype(jnp.int32)
    logits, stats = final_logits(
        assign, token_ids, head_place, rows, over, gain_full, weight_head, width
    )
    stats = spread(stats, ("pipe", "mp"))
    logprobs, chosen = finish(logits, stats.reshape(stats.shape[0], stats.shape[2]))
    return logprobs, chosen[0]


def solution(mesh):
    return jax.shard_map(
        local,
        mesh=mesh,
        in_specs=(
            P(None, "mp"),
            P(),
            P(),
            P(),
            P("pipe", "mp"),
            P("pipe", "mp", None),
            P("pipe", None),
            P("pipe", None, "mp"),
            P("pipe", "mp", None, None, None, None),
            P("mp"),
            P(None, ("pipe", "mp")),
        ),
        out_specs=(P(None, ("pipe", "mp")), P()),
        check_vma=False,
    )
```

```python
import functools

import jax
import jax.numpy as jnp
import numpy as np
from jax import lax
from jax.experimental import pallas as pl
from jax.experimental.pallas import tpu as pltpu
from jax.sharding import PartitionSpec as P

HEADS = 32
KV_HEADS = 4
HEAD_DIM = 128
GROUP = HEADS // KV_HEADS
EPS = 1e-06
THETA = 1000000.0
LANES = 128
CHUNK = 512
OUT_CHUNK = 512
GRANT = 16 * 1024 * 1024

VMEM = pl.BlockSpec(memory_space=pltpu.VMEM)
SMEM = pl.BlockSpec(memory_space=pltpu.SMEM)
HBM = pl.BlockSpec(memory_space=pltpu.HBM)
PARAMS = pltpu.CompilerParams(vmem_limit_bytes=GRANT)


def in_hbm(array):
    return pltpu.with_memory_space_constraint(array, pltpu.HBM)


def in_vmem(array):
    return pltpu.with_memory_space_constraint(array, pltpu.VMEM)


def column_copies(source, target, sem):
    return [
        pltpu.make_async_copy(
            source.at[:, pl.ds(i * CHUNK, CHUNK)], target.at[:, pl.ds(i * CHUNK, CHUNK)], sem.at[i]
        )
        for i in range(target.shape[1] // CHUNK)
    ]


def row_copies(source, target, sem, first):
    return [
        pltpu.make_async_copy(
            source.at[pl.ds(first + i * OUT_CHUNK, OUT_CHUNK)],
            target.at[pl.ds(i * OUT_CHUNK, OUT_CHUNK)],
            sem.at[i],
        )
        for i in range(target.shape[0] // OUT_CHUNK)
    ]


def project_body(stream_ref, gain_ref, weight, out_ref, copies):
    peers, count, _ = out_ref.shape
    current = stream_ref[...].astype(jnp.float32)
    squares = jnp.sum(current * current, axis=1, keepdims=True)
    scaled = (current * gain_ref[...].astype(jnp.float32)).astype(jnp.bfloat16)
    high = squares.astype(jnp.bfloat16).astype(jnp.float32)
    middle = (squares - high).astype(jnp.bfloat16).astype(jnp.float32)
    low = squares - high - middle
    lane = lax.broadcasted_iota(jnp.int32, (current.shape[0], LANES), 1)
    tail = jnp.where(lane == 0, high, jnp.where(lane == 1, middle, jnp.where(lane == 2, low, 0.0)))

    def store(block, at):
        for j in range(peers):
            out_ref[j, :, at : at + block.shape[1]] = block[j * count : (j + 1) * count].astype(
                jnp.bfloat16
            )

    store(tail, weight.shape[1])
    for i in range(weight.shape[1] // CHUNK):
        if copies is not None:
            copies[i].wait()
        block = jnp.dot(
            scaled,
            weight[:, i * CHUNK : (i + 1) * CHUNK],
            preferred_element_type=jnp.float32,
        )
        store(block, i * CHUNK)


def project_first_kernel(
    place_ref, stream_hbm, gain_hbm, source_ref, out_ref, stream_ref, gain_ref, weight_ref, sem
):
    del place_ref
    columns = weight_ref.shape[1] // CHUNK
    copy_stream = pltpu.make_async_copy(stream_hbm, stream_ref, sem.at[columns])
    copy_gain = pltpu.make_async_copy(gain_hbm, gain_ref, sem.at[columns + 1])
    copies = column_copies(source_ref, weight_ref, sem)
    copy_stream.start()
    copy_gain.start()
    for copy in copies:
        copy.start()
    copy_stream.wait()
    copy_gain.wait()
    project_body(stream_ref, gain_ref, weight_ref, out_ref, copies)


def project_kernel(stream_ref, gain_ref, weight_ref, out_ref):
    project_body(stream_ref, gain_ref, weight_ref, out_ref, None)


def project_first(place, stream, gain, weight, peers):
    columns = weight.shape[1]
    count = stream.shape[0] // peers
    return pl.pallas_call(
        project_first_kernel,
        in_specs=[SMEM, HBM, HBM, HBM],
        out_specs=[VMEM, VMEM],
        out_shape=[
            jax.ShapeDtypeStruct((peers, count, columns + LANES), jnp.bfloat16),
            pltpu.VMEM(stream.shape, stream.dtype),
        ],
        scratch_shapes=[
            pltpu.VMEM(gain.shape, gain.dtype),
            pltpu.VMEM(weight.shape, weight.dtype),
            pltpu.SemaphoreType.DMA((columns // CHUNK + 2,)),
        ],
        compiler_params=PARAMS,
        name="project_first",
    )(place, in_hbm(stream), in_hbm(gain), in_hbm(weight))


def load_kernel(order_ref, after_ref, *refs):
    del order_ref, after_ref
    count = len(refs) // 2
    sem = refs[-1]
    copies = [
        pltpu.make_async_copy(
            refs[i].at[pl.ds(0, refs[count + i].shape[0])], refs[count + i], sem.at[i]
        )
        for i in range(count)
    ]
    for copy in copies:
        copy.start()
    for copy in copies:
        copy.wait()


def load(order, after, arrays, rows=None):
    shapes = [array.shape if rows is None else (rows,) + array.shape[1:] for array in arrays]
    size = sum(array.size for array in arrays)
    return pl.pallas_call(
        load_kernel,
        in_specs=[SMEM, VMEM] + [HBM] * len(arrays),
        out_specs=[VMEM] * len(arrays),
        out_shape=[pltpu.VMEM(shape, array.dtype) for shape, array in zip(shapes, arrays)],
        scratch_shapes=[pltpu.SemaphoreType.DMA((len(arrays),))],
        compiler_params=PARAMS,
        cost_estimate=pl.CostEstimate(flops=4 * size, bytes_accessed=4 * size, transcendentals=0),
        name="load",
    )(jnp.full((1,), order, jnp.int32), after, *[in_hbm(array) for array in arrays])


def project(stream, gain, weight, peers):
    columns = weight.shape[1]
    count = stream.shape[0] // peers
    return pl.pallas_call(
        project_kernel,
        in_specs=[VMEM, VMEM, VMEM],
        out_specs=VMEM,
        out_shape=jax.ShapeDtypeStruct((peers, count, columns + LANES), jnp.bfloat16),
        compiler_params=PARAMS,
        name="project",
    )(stream, gain, in_vmem(weight))


def attend_body(lengths_ref, place_ref, parts_ref, bias_ref, frequency_ref, cache, out_ref, width):
    count = out_ref.shape[0]
    length = cache.shape[3]
    query_cols = HEADS * HEAD_DIM
    key_cols = KV_HEADS * HEAD_DIM
    first = place_ref[0] * count
    at_row = lax.broadcasted_iota(jnp.int32, (count, HEAD_DIM), 0)
    positions = jnp.zeros((count, HEAD_DIM), jnp.int32)
    wide = (GROUP * count, count * length)
    rows = lax.broadcasted_iota(jnp.int32, wide, 0) % count
    columns = lax.broadcasted_iota(jnp.int32, wide, 1)
    visible = columns < 0
    for r in range(count):
        position = lengths_ref[first + r]
        positions = jnp.where(at_row == r, position, positions)
        mine = (rows == r) & (columns >= r * length) & (columns < r * length + position)
        visible = visible | mine
    angles = positions.astype(jnp.float32) * frequency_ref[...]
    lane = lax.broadcasted_iota(jnp.int32, (count, HEAD_DIM), 1)
    cosine = jnp.cos(angles)
    sine = jnp.sin(angles)
    sine = jnp.where(lane < HEAD_DIM // 2, -sine, sine)

    def total_of(at, size):
        acc = parts_ref[0, :, at : at + size].astype(jnp.float32)
        for j in range(1, parts_ref.shape[0]):
            acc = acc + parts_ref[j, :, at : at + size].astype(jnp.float32)
        return acc

    squares = jnp.sum(total_of(query_cols + 2 * key_cols, LANES), axis=1, keepdims=True)
    inverse = lax.rsqrt(squares / width + EPS)

    def columns_of(at):
        bias = bias_ref[:, at : at + HEAD_DIM].astype(jnp.float32)
        return total_of(at, HEAD_DIM) * inverse + bias

    def rotate(head):
        return head * cosine + pltpu.roll(head, HEAD_DIM // 2, 1) * sine

    scale = HEAD_DIM ** (-0.5)
    heads = []
    for k in range(KV_HEADS):
        stack = [rotate(columns_of((k * GROUP + g) * HEAD_DIM)) for g in range(GROUP)]
        queries = jnp.concatenate(stack, axis=0).astype(jnp.bfloat16)
        key_new = rotate(columns_of(query_cols + k * HEAD_DIM))
        key_new = key_new.astype(jnp.bfloat16).astype(jnp.float32)
        value_new = columns_of(query_cols + key_cols + k * HEAD_DIM)
        value_new = value_new.astype(jnp.bfloat16).astype(jnp.float32)
        heads.append((queries, key_new, value_new))
    for k in range(KV_HEADS):
        queries, key_new, value_new = heads[k]
        keys = cache[:, 0, k].reshape(count * length, HEAD_DIM)
        values = cache[:, 1, k].reshape(count * length, HEAD_DIM)
        scores = (
            lax.dot_general(
                queries, keys, (((1,), (1,)), ((), ())), preferred_element_type=jnp.float32
            )
            * scale
        )
        tiled_key = jnp.concatenate([key_new] * GROUP, axis=0)
        tiled_value = jnp.concatenate([value_new] * GROUP, axis=0)
        self_score = (
            jnp.sum(queries.astype(jnp.float32) * tiled_key, axis=1, keepdims=True) * scale
        )
        top = jnp.max(jnp.where(visible, scores, -1e30), axis=1, keepdims=True)
        top = jnp.maximum(top, self_score)
        weights = jnp.where(visible, jnp.exp(scores - top), 0.0)
        self_weight = jnp.exp(self_score - top)
        total = jnp.sum(weights, axis=1, keepdims=True) + self_weight
        summed = jnp.dot(weights.astype(jnp.bfloat16), values, preferred_element_type=jnp.float32)
        summed = summed + self_weight.astype(jnp.bfloat16).astype(jnp.float32) * tiled_value
        attended = summed / total
        for g in range(GROUP):
            at = (k * GROUP + g) * HEAD_DIM
            out_ref[:, at : at + HEAD_DIM] = attended[g * count : (g + 1) * count].astype(
                jnp.bfloat16
            )


def attend_kernel(
    lengths_ref, place_ref, parts_ref, bias_ref, frequency_ref, cache_ref, stream_ref, source_ref,
    out_ref, same_ref, weight_ref, sem, *, width,
):
    copies = row_copies(source_ref, weight_ref, sem, 0)
    for copy in copies:
        copy.start()
    same_ref[...] = stream_ref[...]
    attend_body(
        lengths_ref, place_ref, parts_ref, bias_ref, frequency_ref, cache_ref, out_ref, width
    )
    for copy in copies:
        copy.wait()


def attend(lengths, place, parts, bias, frequency, cache, stream, weight, early, width):
    count = parts.shape[1]
    return pl.pallas_call(
        functools.partial(attend_kernel, width=width),
        in_specs=[SMEM, SMEM] + [VMEM] * 5 + [HBM],
        out_specs=[VMEM] * 3,
        out_shape=[
            jax.ShapeDtypeStruct((count, HEADS * HEAD_DIM), jnp.bfloat16),
            jax.ShapeDtypeStruct(stream.shape, stream.dtype),
            pltpu.VMEM((early, weight.shape[1]), weight.dtype),
        ],
        scratch_shapes=[pltpu.SemaphoreType.DMA((early // OUT_CHUNK,))],
        compiler_params=PARAMS,
        name="attend",
    )(lengths, place, parts, bias, frequency, in_vmem(cache), stream, in_hbm(weight))


def combine_kernel(gathered_ref, early_ref, stream_ref, source_ref, out_ref, late_ref, sem):
    early = early_ref.shape[0]
    copies = row_copies(source_ref, late_ref, sem, early)
    for copy in copies:
        copy.start()
    peers = gathered_ref.shape[0]
    blocks = [gathered_ref[j].astype(jnp.float32) for j in range(peers)]
    gathered = jnp.concatenate(blocks, axis=0).astype(jnp.bfloat16)
    update = jnp.dot(gathered[:, :early], early_ref[...], preferred_element_type=jnp.float32)
    for i, copy in enumerate(copies):
        copy.wait()
        at = i * OUT_CHUNK
        update = update + jnp.dot(
            gathered[:, early + at : early + at + OUT_CHUNK],
            late_ref[at : at + OUT_CHUNK],
            preferred_element_type=jnp.float32,
        )
    out_ref[...] = (stream_ref[...].astype(jnp.float32) + update).astype(jnp.bfloat16)


def combine(gathered, early, stream, weight):
    late = weight.shape[0] - early.shape[0]
    return pl.pallas_call(
        combine_kernel,
        in_specs=[VMEM, VMEM, VMEM, HBM],
        out_specs=VMEM,
        out_shape=jax.ShapeDtypeStruct(stream.shape, jnp.bfloat16),
        scratch_shapes=[
            pltpu.VMEM((late, weight.shape[1]), weight.dtype),
            pltpu.SemaphoreType.DMA((late // OUT_CHUNK,)),
        ],
        compiler_params=PARAMS,
        name="combine",
    )(gathered, in_vmem(early), stream, in_hbm(weight))


def logits_kernel(
    assign_ref, tokens_ref, place_ref, rows_ref, over_ref, gain_ref, early_ref, source_ref,
    logits_ref, stats_ref, scratch_ref, late_ref, sem, *, width,
):
    pieces, requests, share = rows_ref.shape
    vocab = early_ref.shape[1]
    early = early_ref.shape[0] // share
    copies = []
    for i in range(pieces - early):
        copies.append(
            pltpu.make_async_copy(
                source_ref.at[pl.ds((early + i) * share, share)],
                late_ref.at[pl.ds(i * share, share)],
                sem.at[i],
            )
        )
        copies[i].start()
    own = place_ref[2] == 1
    squares = jnp.zeros((requests, 1), jnp.float32)
    for m in range(pieces):
        current = jnp.where(own, rows_ref[m], over_ref[m]).astype(jnp.float32)
        squares = squares + jnp.sum(current * current, axis=1, keepdims=True)
    inverse = lax.rsqrt(squares / width + EPS)
    logits = jnp.zeros((requests, vocab), jnp.float32)
    for m in range(pieces):
        current = jnp.where(own, rows_ref[m], over_ref[m]).astype(jnp.float32)
        normed = (current * gain_ref[m].astype(jnp.float32) * inverse).astype(jnp.bfloat16)
        if m < early:
            weight = early_ref[m * share : (m + 1) * share]
        else:
            copies[m - early].wait()
            weight = late_ref[(m - early) * share : (m - early + 1) * share]
        logits = logits + jnp.dot(normed, weight, preferred_element_type=jnp.float32)
    scratch_ref[...] = logits
    row = lax.broadcasted_iota(jnp.int32, (requests, vocab), 0)
    targets = jnp.zeros((requests, vocab), jnp.int32)
    for s in range(requests):
        request = assign_ref[s]
        logits_ref[pl.ds(s, 1), :] = scratch_ref[pl.ds(request, 1), :]
        targets = jnp.where(row == s, tokens_ref[request] - place_ref[1], targets)
    ordered = logits_ref[...]
    column = lax.broadcasted_iota(jnp.int32, (requests, vocab), 1)
    picked = jnp.sum(jnp.where(column == targets, ordered, 0.0), axis=1, keepdims=True)
    top = jnp.max(ordered, axis=1, keepdims=True)
    total = jnp.sum(jnp.exp(ordered - top), axis=1, keepdims=True)
    wide = (requests, stats_ref.shape[1])
    lane = lax.broadcasted_iota(jnp.int32, wide, 1) - lax.broadcasted_iota(jnp.int32, wide, 0)
    spread_out = jnp.where(lane == 0, top, 0.0)
    spread_out = jnp.where(lane == requests, total, spread_out)
    spread_out = jnp.where(lane == 2 * requests, picked, spread_out)
    stats_ref[...] = jnp.sum(spread_out, axis=0, keepdims=True)


def final_logits(assign, tokens, place, rows, over, gain, early, weight, width):
    pieces, requests, share = rows.shape
    vocab = weight.shape[1]
    late = weight.shape[0] - early.shape[0]
    lanes = -(-3 * requests // LANES) * LANES
    return pl.pallas_call(
        functools.partial(logits_kernel, width=width),
        in_specs=[SMEM, SMEM, SMEM, VMEM, VMEM, VMEM, VMEM, HBM],
        out_specs=[VMEM, VMEM],
        out_shape=[
            jax.ShapeDtypeStruct((requests, vocab), jnp.float32),
            jax.ShapeDtypeStruct((1, lanes), jnp.float32),
        ],
        scratch_shapes=[
            pltpu.VMEM((requests, vocab), jnp.float32),
            pltpu.VMEM((late, vocab), weight.dtype),
            pltpu.SemaphoreType.DMA((late // share,)),
        ],
        compiler_params=PARAMS,
        name="final_logits",
    )(assign, tokens, place, rows, over, gain, in_vmem(early), in_hbm(weight))


def finish_kernel(logits_ref, stats_ref, out_ref, chosen_ref):
    requests = logits_ref.shape[0]
    stats = stats_ref[...]
    lanes = stats.shape[1]
    top = jnp.max(stats, axis=0, keepdims=True)
    sums = pltpu.roll(stats, lanes - requests, 1)
    picks = pltpu.roll(stats, lanes - 2 * requests, 1)
    total = jnp.sum(sums * jnp.exp(jnp.minimum(stats - top, 0.0)), axis=0, keepdims=True)
    lane = lax.broadcasted_iota(jnp.int32, (1, lanes), 1)
    total = jnp.where(lane < requests, total, 1.0)
    log_total = jnp.where(lane < requests, top, 0.0) + jnp.log(total)
    chosen_ref[...] = (jnp.sum(picks, axis=0, keepdims=True) - log_total)[:, :requests]
    wide = (requests, lanes)
    here = lax.broadcasted_iota(jnp.int32, wide, 1) == lax.broadcasted_iota(jnp.int32, wide, 0)
    column = jnp.sum(jnp.where(here, log_total, 0.0), axis=1, keepdims=True)
    out_ref[...] = logits_ref[...] - column


def finish(logits, stats):
    requests = logits.shape[0]
    return pl.pallas_call(
        finish_kernel,
        in_specs=[VMEM, VMEM],
        out_specs=[VMEM, VMEM],
        out_shape=[
            jax.ShapeDtypeStruct(logits.shape, jnp.float32),
            jax.ShapeDtypeStruct((1, requests), jnp.float32),
        ],
        compiler_params=PARAMS,
        name="finish",
    )(logits, stats)


def exchange(blocks, axis):
    return lax.all_to_all(blocks, axis, 0, 0, tiled=True)


def spread(value, axis):
    blocks = jnp.broadcast_to(value[None], (lax.axis_size(axis),) + value.shape)
    return exchange(blocks, axis)


def local(
    hidden_in,
    lengths,
    assign,
    token_ids,
    attn_gain,
    qkv_weight,
    qkv_bias,
    out_weight,
    kv_cache,
    final_gain,
    head_weight,
):
    sections = lax.axis_size("pipe")
    section = lax.axis_index("pipe")
    peers = lax.axis_size("mp")
    share = hidden_in.shape[1]
    width = share * peers
    vocab_first = lax.axis_index(("pipe", "mp")) * head_weight.shape[1]
    odd = section % 2 == 1
    place = jnp.stack([lax.axis_index("mp"), vocab_first, odd.astype(vocab_first.dtype)])
    place = place.astype(jnp.int32)
    exponents = np.arange(HEAD_DIM // 2, dtype=np.float64) * 2.0 / HEAD_DIM
    frequency = np.tile(THETA ** (-exponents), 2)[None, :].astype(np.float32)
    weight_in = qkv_weight[0]
    weight_out = out_weight[0]
    cache = kv_cache[0]
    final_row = final_gain[None]

    early = out_weight.shape[1] * 5 // 8 // OUT_CHUNK * OUT_CHUNK

    def run_layer(payload, current, gains, cache_ready):
        parts = exchange(payload, "mp")
        attended, current, early_weight = attend(
            lengths, place, parts, qkv_bias, frequency, cache_ready, current, weight_out, early,
            width,
        )
        return combine(spread(attended, "mp"), early_weight, current, weight_out), gains

    def share_gains(payload, current, gains, *ready):
        return current, spread(final_row, "mp")

    def skip(payload, current, gains, *ready):
        return current, gains

    gain_full = jnp.zeros((peers, 1, share), final_gain.dtype)
    for layer in range(sections):
        active = section == layer
        if layer == 0:
            payload, stream = project_first(place, hidden_in, attn_gain, weight_in, peers)
            branch = jnp.where(active, 0, 1)
            branches = (run_layer, share_gains)
            ready = [cache]
        else:
            payload = project(stream, attn_gain, in_ready, peers)
            branch = jnp.where(active, 1, jnp.where(section == 0, 2, 0) if layer == 1 else 0)
            branches = (skip, run_layer, share_gains) if layer == 1 else (skip, run_layer)
        stream, gain_full = lax.switch(branch, branches, payload, stream, gain_full, *ready)
        if layer + 1 < sections:
            in_ready, *ready = load(layer, stream, [weight_in, cache])
            stream = lax.ppermute(stream, "pipe", [(layer, layer + 1)])

    last = sections - 1
    arrived = stream
    for target in range(1, last, 2):
        copied = lax.ppermute(stream, "pipe", [(last, target)])
        arrived = jnp.where(section == target, copied, arrived)
    rows = lax.cond(
        odd,
        lambda b: spread(b, "mp"),
        lambda b: jnp.broadcast_to(b[None], (peers,) + b.shape),
        arrived,
    )
    (head_ready,) = load(sections, rows, [head_weight], width * 3 // 4)
    over = lax.ppermute(rows, "pipe", [(i, i - 1) for i in range(1, sections, 2)])

    logits, stats = final_logits(
        assign, token_ids, place, rows, over, gain_full, head_ready, head_weight, width
    )
    stats = spread(stats, ("pipe", "mp"))
    logprobs, chosen = finish(logits, stats.reshape(stats.shape[0], stats.shape[2]))
    return logprobs, chosen[0]


def solution(mesh):
    return jax.shard_map(
        local,
        mesh=mesh,
        in_specs=(
            P(None, "mp"),
            P(),
            P(),
            P(),
            P("pipe", "mp"),
            P("pipe", "mp", None),
            P("pipe", None),
            P("pipe", None, "mp"),
            P("pipe", "mp", None, None, None, None),
            P("mp"),
            P(None, ("pipe", "mp")),
        ),
        out_specs=(P(None, ("pipe", "mp")), P()),
        check_vma=False,
    )
```

```python
import functools

import jax
import jax.numpy as jnp
import numpy as np
from jax import lax
from jax.experimental import pallas as pl
from jax.experimental.pallas import tpu as pltpu
from jax.sharding import PartitionSpec as P

HEADS = 32
KV_HEADS = 4
HEAD_DIM = 128
GROUP = HEADS // KV_HEADS
EPS = 1e-06
THETA = 1000000.0
LANES = 128
CHUNK = 512
OUT_CHUNK = 256
COVER = 32
GRANT = 16 * 1024 * 1024
FULL_GRANT = 60 * 1024 * 1024

VMEM = pl.BlockSpec(memory_space=pltpu.VMEM)
SMEM = pl.BlockSpec(memory_space=pltpu.SMEM)
HBM = pl.BlockSpec(memory_space=pltpu.HBM)
PARAMS = pltpu.CompilerParams(vmem_limit_bytes=GRANT)


def in_hbm(array):
    return pltpu.with_memory_space_constraint(array, pltpu.HBM)


def in_vmem(array):
    return pltpu.with_memory_space_constraint(array, pltpu.VMEM)


def column_copies(source, target, sem):
    return [
        pltpu.make_async_copy(
            source.at[:, pl.ds(i * CHUNK, CHUNK)], target.at[:, pl.ds(i * CHUNK, CHUNK)], sem.at[i]
        )
        for i in range(target.shape[1] // CHUNK)
    ]


def project_body(stream_ref, gain_ref, weight, out_ref, copies):
    peers, count, _ = out_ref.shape
    current = stream_ref[...].astype(jnp.float32)
    squares = jnp.sum(current * current, axis=1, keepdims=True)
    scaled = (current * gain_ref[...].astype(jnp.float32)).astype(jnp.bfloat16)
    high = squares.astype(jnp.bfloat16).astype(jnp.float32)
    middle = (squares - high).astype(jnp.bfloat16).astype(jnp.float32)
    low = squares - high - middle
    lane = lax.broadcasted_iota(jnp.int32, (current.shape[0], LANES), 1)
    tail = jnp.where(lane == 0, high, jnp.where(lane == 1, middle, jnp.where(lane == 2, low, 0.0)))

    def store(block, at):
        for j in range(peers):
            out_ref[j, :, at : at + block.shape[1]] = block[j * count : (j + 1) * count].astype(
                jnp.bfloat16
            )

    store(tail, weight.shape[1])
    for i in range(weight.shape[1] // CHUNK):
        if copies is not None:
            copies[i].wait()
        block = jnp.dot(
            scaled,
            weight[:, i * CHUNK : (i + 1) * CHUNK],
            preferred_element_type=jnp.float32,
        )
        store(block, i * CHUNK)


def project_first_kernel(
    place_ref, stream_hbm, gain_hbm, source_ref, out_ref, stream_ref, gain_ref, weight_ref, sem
):
    del place_ref
    columns = weight_ref.shape[1] // CHUNK
    copy_stream = pltpu.make_async_copy(stream_hbm, stream_ref, sem.at[columns])
    copy_gain = pltpu.make_async_copy(gain_hbm, gain_ref, sem.at[columns + 1])
    copies = column_copies(source_ref, weight_ref, sem)
    copy_stream.start()
    copy_gain.start()
    for copy in copies:
        copy.start()
    copy_stream.wait()
    copy_gain.wait()
    project_body(stream_ref, gain_ref, weight_ref, out_ref, copies)


def project_kernel(stream_ref, gain_ref, weight_ref, out_ref):
    project_body(stream_ref, gain_ref, weight_ref, out_ref, None)


def project_first(place, stream, gain, weight, peers):
    columns = weight.shape[1]
    count = stream.shape[0] // peers
    return pl.pallas_call(
        project_first_kernel,
        in_specs=[SMEM, HBM, HBM, HBM],
        out_specs=[VMEM, VMEM],
        out_shape=[
            jax.ShapeDtypeStruct((peers, count, columns + LANES), jnp.bfloat16),
            pltpu.VMEM(stream.shape, stream.dtype),
        ],
        scratch_shapes=[
            pltpu.VMEM(gain.shape, gain.dtype),
            pltpu.VMEM(weight.shape, weight.dtype),
            pltpu.SemaphoreType.DMA((columns // CHUNK + 2,)),
        ],
        compiler_params=pltpu.CompilerParams(vmem_limit_bytes=FULL_GRANT),
        name="project_first",
    )(place, in_hbm(stream), in_hbm(gain), in_hbm(weight))


def load_kernel(order_ref, after_ref, *refs):
    del order_ref, after_ref
    count = len(refs) // 2
    sem = refs[-1]
    copies = [
        pltpu.make_async_copy(
            refs[i].at[pl.ds(0, refs[count + i].shape[0])], refs[count + i], sem.at[i]
        )
        for i in range(count)
    ]
    for copy in copies:
        copy.start()
    for copy in copies:
        copy.wait()


def load(order, after, arrays, rows=None):
    shapes = [array.shape if rows is None else (rows,) + array.shape[1:] for array in arrays]
    size = sum(array.size for array in arrays)
    return pl.pallas_call(
        load_kernel,
        in_specs=[SMEM, VMEM] + [HBM] * len(arrays),
        out_specs=[VMEM] * len(arrays),
        out_shape=[pltpu.VMEM(shape, array.dtype) for shape, array in zip(shapes, arrays)],
        scratch_shapes=[pltpu.SemaphoreType.DMA((len(arrays),))],
        compiler_params=PARAMS,
        cost_estimate=pl.CostEstimate(flops=4 * size, bytes_accessed=4 * size, transcendentals=0),
        name="load",
    )(jnp.full((1,), order, jnp.int32), after, *[in_hbm(array) for array in arrays])


def project(stream, gain, weight, peers):
    columns = weight.shape[1]
    count = stream.shape[0] // peers
    return pl.pallas_call(
        project_kernel,
        in_specs=[VMEM, VMEM, VMEM],
        out_specs=VMEM,
        out_shape=jax.ShapeDtypeStruct((peers, count, columns + LANES), jnp.bfloat16),
        compiler_params=PARAMS,
        name="project",
    )(stream, gain, in_vmem(weight))


def attend_body(lengths_ref, place_ref, parts_ref, bias_ref, frequency_ref, cache, out_ref, width):
    count = out_ref.shape[0]
    length = cache.shape[3]
    query_cols = HEADS * HEAD_DIM
    key_cols = KV_HEADS * HEAD_DIM
    first = place_ref[0] * count
    at_row = lax.broadcasted_iota(jnp.int32, (count, HEAD_DIM), 0)
    positions = jnp.zeros((count, HEAD_DIM), jnp.int32)
    wide = (GROUP * count, count * length)
    rows = lax.broadcasted_iota(jnp.int32, wide, 0) % count
    columns = lax.broadcasted_iota(jnp.int32, wide, 1)
    visible = columns < 0
    for r in range(count):
        position = lengths_ref[first + r]
        positions = jnp.where(at_row == r, position, positions)
        mine = (rows == r) & (columns >= r * length) & (columns < r * length + position)
        visible = visible | mine
    angles = positions.astype(jnp.float32) * frequency_ref[...]
    lane = lax.broadcasted_iota(jnp.int32, (count, HEAD_DIM), 1)
    cosine = jnp.cos(angles)
    sine = jnp.sin(angles)
    sine = jnp.where(lane < HEAD_DIM // 2, -sine, sine)

    def total_of(at, size):
        acc = parts_ref[0, :, at : at + size].astype(jnp.float32)
        for j in range(1, parts_ref.shape[0]):
            acc = acc + parts_ref[j, :, at : at + size].astype(jnp.float32)
        return acc

    squares = jnp.sum(total_of(query_cols + 2 * key_cols, LANES), axis=1, keepdims=True)
    inverse = lax.rsqrt(squares / width + EPS)

    def columns_of(at):
        bias = bias_ref[:, at : at + HEAD_DIM].astype(jnp.float32)
        return total_of(at, HEAD_DIM) * inverse + bias

    def rotate(head):
        return head * cosine + pltpu.roll(head, HEAD_DIM // 2, 1) * sine

    scale = HEAD_DIM ** (-0.5)
    heads = []
    for k in range(KV_HEADS):
        stack = [rotate(columns_of((k * GROUP + g) * HEAD_DIM)) for g in range(GROUP)]
        queries = jnp.concatenate(stack, axis=0).astype(jnp.bfloat16)
        key_new = rotate(columns_of(query_cols + k * HEAD_DIM))
        key_new = key_new.astype(jnp.bfloat16).astype(jnp.float32)
        value_new = columns_of(query_cols + key_cols + k * HEAD_DIM)
        value_new = value_new.astype(jnp.bfloat16).astype(jnp.float32)
        heads.append((queries, key_new, value_new))
    for k in range(KV_HEADS):
        queries, key_new, value_new = heads[k]
        keys = cache[:, 0, k].reshape(count * length, HEAD_DIM)
        values = cache[:, 1, k].reshape(count * length, HEAD_DIM)
        scores = (
            lax.dot_general(
                queries, keys, (((1,), (1,)), ((), ())), preferred_element_type=jnp.float32
            )
            * scale
        )
        tiled_key = jnp.concatenate([key_new] * GROUP, axis=0)
        tiled_value = jnp.concatenate([value_new] * GROUP, axis=0)
        self_score = (
            jnp.sum(queries.astype(jnp.float32) * tiled_key, axis=1, keepdims=True) * scale
        )
        top = jnp.max(jnp.where(visible, scores, -1e30), axis=1, keepdims=True)
        top = jnp.maximum(top, self_score)
        weights = jnp.where(visible, jnp.exp(scores - top), 0.0)
        self_weight = jnp.exp(self_score - top)
        total = jnp.sum(weights, axis=1, keepdims=True) + self_weight
        summed = jnp.dot(weights.astype(jnp.bfloat16), values, preferred_element_type=jnp.float32)
        summed = summed + self_weight.astype(jnp.bfloat16).astype(jnp.float32) * tiled_value
        attended = summed / total
        for g in range(GROUP):
            at = (k * GROUP + g) * HEAD_DIM
            out_ref[:, at : at + HEAD_DIM] = attended[g * count : (g + 1) * count].astype(
                jnp.bfloat16
            )


def attend_kernel(
    lengths_ref, place_ref, parts_ref, bias_ref, frequency_ref, cache_ref, stream_ref,
    out_ref, same_ref, *, width,
):
    same_ref[...] = stream_ref[...]
    attend_body(
        lengths_ref, place_ref, parts_ref, bias_ref, frequency_ref, cache_ref, out_ref, width
    )


def attend(lengths, place, parts, bias, frequency, cache, stream, width):
    count = parts.shape[1]
    return pl.pallas_call(
        functools.partial(attend_kernel, width=width),
        in_specs=[SMEM, SMEM] + [VMEM] * 5,
        out_specs=[VMEM] * 2,
        out_shape=[
            jax.ShapeDtypeStruct((count, HEADS * HEAD_DIM), jnp.bfloat16),
            jax.ShapeDtypeStruct(stream.shape, stream.dtype),
        ],
        compiler_params=PARAMS,
        cost_estimate=pl.CostEstimate(
            flops=COVER * stream.size * HEADS * HEAD_DIM, bytes_accessed=cache.size * 2, transcendentals=0
        ),
        name="attend",
    )(lengths, place, parts, bias, frequency, in_vmem(cache), stream)


def combine_kernel(gathered_ref, weight_ref, stream_ref, out_ref):
    peers = gathered_ref.shape[0]
    blocks = [gathered_ref[j].astype(jnp.float32) for j in range(peers)]
    gathered = jnp.concatenate(blocks, axis=0).astype(jnp.bfloat16)
    for at in range(0, out_ref.shape[1], OUT_CHUNK):
        update = jnp.dot(
            gathered, weight_ref[:, at : at + OUT_CHUNK], preferred_element_type=jnp.float32
        )
        current = stream_ref[:, at : at + OUT_CHUNK].astype(jnp.float32)
        out_ref[:, at : at + OUT_CHUNK] = (current + update).astype(jnp.bfloat16)


def combine(gathered, weight, stream):
    return pl.pallas_call(
        combine_kernel,
        in_specs=[VMEM, VMEM, VMEM],
        out_specs=VMEM,
        out_shape=jax.ShapeDtypeStruct(stream.shape, jnp.bfloat16),
        compiler_params=PARAMS,
        name="combine",
    )(gathered, in_vmem(weight), stream)


def logits_kernel(
    assign_ref, tokens_ref, place_ref, rows_ref, over_ref, gain_ref, early_ref, source_ref,
    logits_ref, stats_ref, scratch_ref, late_ref, sem, *, width,
):
    pieces, requests, share = rows_ref.shape
    vocab = early_ref.shape[1]
    early = early_ref.shape[0] // share
    copies = []
    for i in range(pieces - early):
        copies.append(
            pltpu.make_async_copy(
                source_ref.at[pl.ds((early + i) * share, share)],
                late_ref.at[pl.ds(i * share, share)],
                sem.at[i],
            )
        )
        copies[i].start()
    own = place_ref[2] == 1
    squares = jnp.zeros((requests, 1), jnp.float32)
    for m in range(pieces):
        current = jnp.where(own, rows_ref[m], over_ref[m]).astype(jnp.float32)
        squares = squares + jnp.sum(current * current, axis=1, keepdims=True)
    inverse = lax.rsqrt(squares / width + EPS)
    logits = jnp.zeros((requests, vocab), jnp.float32)
    for m in range(pieces):
        current = jnp.where(own, rows_ref[m], over_ref[m]).astype(jnp.float32)
        normed = (current * gain_ref[m].astype(jnp.float32) * inverse).astype(jnp.bfloat16)
        if m < early:
            weight = early_ref[m * share : (m + 1) * share]
        else:
            copies[m - early].wait()
            weight = late_ref[(m - early) * share : (m - early + 1) * share]
        logits = logits + jnp.dot(normed, weight, preferred_element_type=jnp.float32)
    scratch_ref[...] = logits
    row = lax.broadcasted_iota(jnp.int32, (requests, vocab), 0)
    targets = jnp.zeros((requests, vocab), jnp.int32)
    for s in range(requests):
        request = assign_ref[s]
        logits_ref[pl.ds(s, 1), :] = scratch_ref[pl.ds(request, 1), :]
        targets = jnp.where(row == s, tokens_ref[request] - place_ref[1], targets)
    ordered = logits_ref[...]
    column = lax.broadcasted_iota(jnp.int32, (requests, vocab), 1)
    picked = jnp.sum(jnp.where(column == targets, ordered, 0.0), axis=1, keepdims=True)
    top = jnp.max(ordered, axis=1, keepdims=True)
    total = jnp.sum(jnp.exp(ordered - top), axis=1, keepdims=True)
    wide = (requests, stats_ref.shape[1])
    lane = lax.broadcasted_iota(jnp.int32, wide, 1) - lax.broadcasted_iota(jnp.int32, wide, 0)
    spread_out = jnp.where(lane == 0, top, 0.0)
    spread_out = jnp.where(lane == requests, total, spread_out)
    spread_out = jnp.where(lane == 2 * requests, picked, spread_out)
    stats_ref[...] = jnp.sum(spread_out, axis=0, keepdims=True)


def final_logits(assign, tokens, place, rows, over, gain, early, weight, width):
    pieces, requests, share = rows.shape
    vocab = weight.shape[1]
    late = weight.shape[0] - early.shape[0]
    lanes = -(-3 * requests // LANES) * LANES
    return pl.pallas_call(
        functools.partial(logits_kernel, width=width),
        in_specs=[SMEM, SMEM, SMEM, VMEM, VMEM, VMEM, VMEM, HBM],
        out_specs=[VMEM, VMEM],
        out_shape=[
            jax.ShapeDtypeStruct((requests, vocab), jnp.float32),
            jax.ShapeDtypeStruct((1, lanes), jnp.float32),
        ],
        scratch_shapes=[
            pltpu.VMEM((requests, vocab), jnp.float32),
            pltpu.VMEM((late, vocab), weight.dtype),
            pltpu.SemaphoreType.DMA((late // share,)),
        ],
        compiler_params=PARAMS,
        name="final_logits",
    )(assign, tokens, place, rows, over, gain, in_vmem(early), in_hbm(weight))


def finish_kernel(logits_ref, stats_ref, out_ref, chosen_ref):
    requests = logits_ref.shape[0]
    stats = stats_ref[...]
    lanes = stats.shape[1]
    top = jnp.max(stats, axis=0, keepdims=True)
    sums = pltpu.roll(stats, lanes - requests, 1)
    picks = pltpu.roll(stats, lanes - 2 * requests, 1)
    total = jnp.sum(sums * jnp.exp(jnp.minimum(stats - top, 0.0)), axis=0, keepdims=True)
    lane = lax.broadcasted_iota(jnp.int32, (1, lanes), 1)
    total = jnp.where(lane < requests, total, 1.0)
    log_total = jnp.where(lane < requests, top, 0.0) + jnp.log(total)
    chosen_ref[...] = (jnp.sum(picks, axis=0, keepdims=True) - log_total)[:, :requests]
    wide = (requests, lanes)
    here = lax.broadcasted_iota(jnp.int32, wide, 1) == lax.broadcasted_iota(jnp.int32, wide, 0)
    column = jnp.sum(jnp.where(here, log_total, 0.0), axis=1, keepdims=True)
    out_ref[...] = logits_ref[...] - column


def finish(logits, stats):
    requests = logits.shape[0]
    return pl.pallas_call(
        finish_kernel,
        in_specs=[VMEM, VMEM],
        out_specs=[VMEM, VMEM],
        out_shape=[
            jax.ShapeDtypeStruct(logits.shape, jnp.float32),
            jax.ShapeDtypeStruct((1, requests), jnp.float32),
        ],
        compiler_params=PARAMS,
        name="finish",
    )(logits, stats)


def exchange(blocks, axis):
    return lax.all_to_all(blocks, axis, 0, 0, tiled=True)


def spread(value, axis):
    blocks = jnp.broadcast_to(value[None], (lax.axis_size(axis),) + value.shape)
    return exchange(blocks, axis)


def local(
    hidden_in,
    lengths,
    assign,
    token_ids,
    attn_gain,
    qkv_weight,
    qkv_bias,
    out_weight,
    kv_cache,
    final_gain,
    head_weight,
):
    sections = lax.axis_size("pipe")
    section = lax.axis_index("pipe")
    peers = lax.axis_size("mp")
    share = hidden_in.shape[1]
    width = share * peers
    vocab_first = lax.axis_index(("pipe", "mp")) * head_weight.shape[1]
    odd = section % 2 == 1
    place = jnp.stack([lax.axis_index("mp"), vocab_first, odd.astype(vocab_first.dtype)])
    place = place.astype(jnp.int32)
    exponents = np.arange(HEAD_DIM // 2, dtype=np.float64) * 2.0 / HEAD_DIM
    frequency = np.tile(THETA ** (-exponents), 2)[None, :].astype(np.float32)
    weight_in = qkv_weight[0]
    weight_out = out_weight[0]
    cache = kv_cache[0]
    final_row = final_gain[None]

    def run_layer(payload, current, gains, cache_ready):
        parts = exchange(payload, "mp")
        attended, current = attend(
            lengths, place, parts, qkv_bias, frequency, cache_ready, current, width
        )
        return combine(spread(attended, "mp"), weight_out, current), gains

    def share_gains(payload, current, gains, *ready):
        return current, spread(final_row, "mp")

    def skip(payload, current, gains, *ready):
        return current, gains

    gain_full = jnp.zeros((peers, 1, share), final_gain.dtype)
    for layer in range(sections):
        active = section == layer
        if layer == 0:
            payload, stream = project_first(place, hidden_in, attn_gain, weight_in, peers)
            branch = jnp.where(active, 0, 1)
            branches = (run_layer, share_gains)
            ready = [cache]
        else:
            payload = project(stream, attn_gain, in_ready, peers)
            branch = jnp.where(active, 1, jnp.where(section == 0, 2, 0) if layer == 1 else 0)
            branches = (skip, run_layer, share_gains) if layer == 1 else (skip, run_layer)
        stream, gain_full = lax.switch(branch, branches, payload, stream, gain_full, *ready)
        if layer + 1 < sections:
            in_ready, *ready = load(layer, stream, [weight_in, cache])
            stream = lax.ppermute(stream, "pipe", [(layer, layer + 1)])

    last = sections - 1
    arrived = stream
    for target in range(1, last, 2):
        copied = lax.ppermute(stream, "pipe", [(last, target)])
        arrived = jnp.where(section == target, copied, arrived)
    rows = lax.cond(
        odd,
        lambda b: spread(b, "mp"),
        lambda b: jnp.broadcast_to(b[None], (peers,) + b.shape),
        arrived,
    )
    (head_ready,) = load(sections, rows, [head_weight], width * 3 // 4)
    over = lax.ppermute(rows, "pipe", [(i, i - 1) for i in range(1, sections, 2)])

    logits, stats = final_logits(
        assign, token_ids, place, rows, over, gain_full, head_ready, head_weight, width
    )
    stats = spread(stats, ("pipe", "mp"))
    logprobs, chosen = finish(logits, stats.reshape(stats.shape[0], stats.shape[2]))
    return logprobs, chosen[0]


def solution(mesh):
    return jax.shard_map(
        local,
        mesh=mesh,
        in_specs=(
            P(None, "mp"),
            P(),
            P(),
            P(),
            P("pipe", "mp"),
            P("pipe", "mp", None),
            P("pipe", None),
            P("pipe", None, "mp"),
            P("pipe", "mp", None, None, None, None),
            P("mp"),
            P(None, ("pipe", "mp")),
        ),
        out_specs=(P(None, ("pipe", "mp")), P()),
        check_vma=False,
    )
```

```python
import functools

import jax
import jax.numpy as jnp
import numpy as np
from jax import lax
from jax.experimental import pallas as pl
from jax.experimental.pallas import tpu as pltpu
from jax.sharding import PartitionSpec as P


HEADS = 32
KV_HEADS = 4
HEAD_DIM = 128
GROUP = HEADS // KV_HEADS
EPS = 1e-06
THETA = 1000000.0
LANES = 128
CHUNK = 512
OUT_CHUNK = 256
COVER = 128
RELAY_PIECES = 4
GRANT = 10 * 1024 * 1024
FULL_GRANT = 60 * 1024 * 1024

VMEM = pl.BlockSpec(memory_space=pltpu.VMEM)
SMEM = pl.BlockSpec(memory_space=pltpu.SMEM)
HBM = pl.BlockSpec(memory_space=pltpu.HBM)
PARAMS = pltpu.CompilerParams(vmem_limit_bytes=GRANT)


def in_hbm(array):
    return pltpu.with_memory_space_constraint(array, pltpu.HBM)


def in_vmem(array):
    return pltpu.with_memory_space_constraint(array, pltpu.VMEM)


def column_copies(source, target, sem):
    return [
        pltpu.make_async_copy(
            source.at[:, pl.ds(i * CHUNK, CHUNK)], target.at[:, pl.ds(i * CHUNK, CHUNK)], sem.at[i]
        )
        for i in range(target.shape[1] // CHUNK)
    ]


def project_body(stream_ref, gain_ref, weight, out_ref, copies):
    peers, count, _ = out_ref.shape
    current = stream_ref[...].astype(jnp.float32)
    squares = jnp.sum(current * current, axis=1, keepdims=True)
    scaled = (current * gain_ref[:, : stream_ref.shape[1]].astype(jnp.float32)).astype(jnp.bfloat16)
    high = squares.astype(jnp.bfloat16).astype(jnp.float32)
    middle = (squares - high).astype(jnp.bfloat16).astype(jnp.float32)
    low = squares - high - middle
    lane = lax.broadcasted_iota(jnp.int32, (current.shape[0], LANES), 1)
    tail = jnp.where(lane == 0, high, jnp.where(lane == 1, middle, jnp.where(lane == 2, low, 0.0)))

    def store(block, at):
        for j in range(peers):
            out_ref[j, :, at : at + block.shape[1]] = block[j * count : (j + 1) * count].astype(
                jnp.bfloat16
            )

    store(tail, weight.shape[1])
    for i in range(weight.shape[1] // CHUNK):
        if copies is not None:
            copies[i].wait()
        block = jnp.dot(
            scaled,
            weight[:, i * CHUNK : (i + 1) * CHUNK],
            preferred_element_type=jnp.float32,
        )
        store(block, i * CHUNK)


def project_first_kernel(
    place_ref, stream_hbm, gain_hbm, source_ref, cache_hbm,
    out_ref, stream_ref, cache_ref, gain_ref, weight_ref, sem,
):
    del place_ref
    columns = weight_ref.shape[1] // CHUNK
    copy_stream = pltpu.make_async_copy(stream_hbm, stream_ref, sem.at[columns])
    copy_gain = pltpu.make_async_copy(gain_hbm, gain_ref, sem.at[columns + 1])
    copies = column_copies(source_ref, weight_ref, sem)
    copy_stream.start()
    copy_gain.start()
    for copy in copies:
        copy.start()
    copy_cache = pltpu.make_async_copy(cache_hbm, cache_ref, sem.at[columns + 2])
    copy_cache.start()
    copy_stream.wait()
    copy_gain.wait()
    project_body(stream_ref, gain_ref, weight_ref, out_ref, copies)
    copy_cache.wait()


def project_kernel(stream_ref, gain_ref, weight_ref, out_ref):
    project_body(stream_ref, gain_ref, weight_ref, out_ref, None)


def project_first(place, stream, gain, weight, cache, peers):
    columns = weight.shape[1]
    count = stream.shape[0] // peers
    return pl.pallas_call(
        project_first_kernel,
        in_specs=[SMEM] + [HBM] * 4,
        out_specs=[VMEM] * 3,
        out_shape=[
            jax.ShapeDtypeStruct((peers, count, columns + LANES), jnp.bfloat16),
            pltpu.VMEM(stream.shape, stream.dtype),
            pltpu.VMEM(cache.shape, cache.dtype),
        ],
        scratch_shapes=[
            pltpu.VMEM(gain.shape, gain.dtype),
            pltpu.VMEM(weight.shape, weight.dtype),
            pltpu.SemaphoreType.DMA((columns // CHUNK + 3,)),
        ],
        compiler_params=pltpu.CompilerParams(vmem_limit_bytes=FULL_GRANT),
        name="project_first",
    )(place, in_hbm(stream), in_hbm(gain), in_hbm(weight), in_hbm(cache))


def load_kernel(order_ref, after_ref, *refs):
    del order_ref, after_ref
    count = len(refs) // 2
    sem = refs[-1]
    copies = [
        pltpu.make_async_copy(
            refs[i].at[pl.ds(0, refs[count + i].shape[0])], refs[count + i], sem.at[i]
        )
        for i in range(count)
    ]
    for copy in copies:
        copy.start()
    for copy in copies:
        copy.wait()


def load(order, after, arrays, rows=None):
    shapes = [array.shape if rows is None else (rows,) + array.shape[1:] for array in arrays]
    size = sum(array.size for array in arrays)
    return pl.pallas_call(
        load_kernel,
        in_specs=[SMEM, VMEM] + [HBM] * len(arrays),
        out_specs=[VMEM] * len(arrays),
        out_shape=[pltpu.VMEM(shape, array.dtype) for shape, array in zip(shapes, arrays)],
        scratch_shapes=[pltpu.SemaphoreType.DMA((len(arrays),))],
        compiler_params=PARAMS,
        cost_estimate=pl.CostEstimate(flops=4 * size, bytes_accessed=4 * size, transcendentals=0),
        name="load",
    )(jnp.full((1,), order, jnp.int32), after, *[in_hbm(array) for array in arrays])


def relay_kernel(source_ref, out_ref, buffer_ref, sem_in, sem_out):
    pieces = sem_in.shape[0]
    size = source_ref.shape[0] // pieces
    spans = [pl.ds(i * size, size) for i in range(pieces)]
    arrive = [
        pltpu.make_async_copy(source_ref.at[span], buffer_ref.at[span], sem_in.at[i])
        for i, span in enumerate(spans)
    ]
    leave = [
        pltpu.make_async_copy(buffer_ref.at[span], out_ref.at[span], sem_out.at[i])
        for i, span in enumerate(spans)
    ]
    for copy in arrive:
        copy.start()
    for i in range(pieces):
        arrive[i].wait()
        leave[i].start()
    for copy in leave:
        copy.wait()


def relay(array):
    return pl.pallas_call(
        relay_kernel,
        in_specs=[HBM],
        out_specs=pl.BlockSpec(memory_space=pl.ANY),
        out_shape=jax.ShapeDtypeStruct(array.shape, array.dtype),
        scratch_shapes=[
            pltpu.VMEM(array.shape, array.dtype),
            pltpu.SemaphoreType.DMA((RELAY_PIECES,)),
            pltpu.SemaphoreType.DMA((RELAY_PIECES,)),
        ],
        compiler_params=PARAMS,
        cost_estimate=pl.CostEstimate(
            flops=4 * array.size, bytes_accessed=4 * array.size, transcendentals=0
        ),
        name="relay",
    )(in_hbm(array))


def project(stream, gain, weight, peers):
    columns = weight.shape[1]
    count = stream.shape[0] // peers
    return pl.pallas_call(
        project_kernel,
        in_specs=[VMEM, VMEM, VMEM],
        out_specs=VMEM,
        out_shape=jax.ShapeDtypeStruct((peers, count, columns + LANES), jnp.bfloat16),
        compiler_params=PARAMS,
        name="project",
    )(stream, gain, in_vmem(weight))


def project_load_kernel(stream_ref, gain_ref, weight_ref, cache_hbm, out_ref, cache_ref, sem):
    copy = pltpu.make_async_copy(cache_hbm, cache_ref, sem.at[0])
    copy.start()
    project_body(stream_ref, gain_ref, weight_ref, out_ref, None)
    copy.wait()


def project_load(stream, gain, weight, cache, peers):
    columns = weight.shape[1]
    count = stream.shape[0] // peers
    return pl.pallas_call(
        project_load_kernel,
        in_specs=[VMEM, VMEM, VMEM, HBM],
        out_specs=[VMEM, VMEM],
        out_shape=[
            jax.ShapeDtypeStruct((peers, count, columns + LANES), jnp.bfloat16),
            pltpu.VMEM(cache.shape, cache.dtype),
        ],
        scratch_shapes=[pltpu.SemaphoreType.DMA((1,))],
        compiler_params=PARAMS,
        name="project_load",
    )(stream, gain, in_vmem(weight), in_hbm(cache))


def attend_body(lengths_ref, place_ref, parts_ref, bias_ref, frequency_ref, cache, out_ref, width):
    count = out_ref.shape[0]
    length = cache.shape[3]
    query_cols = HEADS * HEAD_DIM
    key_cols = KV_HEADS * HEAD_DIM
    first = place_ref[0] * count
    at_row = lax.broadcasted_iota(jnp.int32, (count, HEAD_DIM), 0)
    positions = jnp.zeros((count, HEAD_DIM), jnp.int32)
    wide = (GROUP * count, count * length)
    rows = lax.broadcasted_iota(jnp.int32, wide, 0) % count
    columns = lax.broadcasted_iota(jnp.int32, wide, 1)
    visible = columns < 0
    for r in range(count):
        position = lengths_ref[first + r]
        positions = jnp.where(at_row == r, position, positions)
        mine = (rows == r) & (columns >= r * length) & (columns < r * length + position)
        visible = visible | mine
    angles = positions.astype(jnp.float32) * frequency_ref[...]
    lane = lax.broadcasted_iota(jnp.int32, (count, HEAD_DIM), 1)
    cosine = jnp.cos(angles)
    sine = jnp.sin(angles)
    sine = jnp.where(lane < HEAD_DIM // 2, -sine, sine)

    def total_of(at, size):
        acc = parts_ref[0, :, at : at + size].astype(jnp.float32)
        for j in range(1, parts_ref.shape[0]):
            acc = acc + parts_ref[j, :, at : at + size].astype(jnp.float32)
        return acc

    squares = jnp.sum(total_of(query_cols + 2 * key_cols, LANES), axis=1, keepdims=True)
    inverse = lax.rsqrt(squares / width + EPS)

    def columns_of(at):
        shifted = at + bias_ref.shape[1] - (query_cols + 2 * key_cols)
        bias = bias_ref[:, shifted : shifted + HEAD_DIM].astype(jnp.float32)
        return total_of(at, HEAD_DIM) * inverse + bias

    def rotate(head):
        return head * cosine + pltpu.roll(head, HEAD_DIM // 2, 1) * sine

    scale = HEAD_DIM ** (-0.5)
    heads = []
    for k in range(KV_HEADS):
        stack = [rotate(columns_of((k * GROUP + g) * HEAD_DIM)) for g in range(GROUP)]
        queries = jnp.concatenate(stack, axis=0).astype(jnp.bfloat16)
        key_new = rotate(columns_of(query_cols + k * HEAD_DIM))
        key_new = key_new.astype(jnp.bfloat16).astype(jnp.float32)
        value_new = columns_of(query_cols + key_cols + k * HEAD_DIM)
        value_new = value_new.astype(jnp.bfloat16).astype(jnp.float32)
        heads.append((queries, key_new, value_new))
    for k in range(KV_HEADS):
        queries, key_new, value_new = heads[k]
        keys = cache[:, 0, k].reshape(count * length, HEAD_DIM)
        values = cache[:, 1, k].reshape(count * length, HEAD_DIM)
        scores = (
            lax.dot_general(
                queries, keys, (((1,), (1,)), ((), ())), preferred_element_type=jnp.float32
            )
            * scale
        )
        tiled_key = jnp.concatenate([key_new] * GROUP, axis=0)
        tiled_value = jnp.concatenate([value_new] * GROUP, axis=0)
        self_score = (
            jnp.sum(queries.astype(jnp.float32) * tiled_key, axis=1, keepdims=True) * scale
        )
        top = jnp.max(jnp.where(visible, scores, -1e30), axis=1, keepdims=True)
        top = jnp.maximum(top, self_score)
        weights = jnp.where(visible, jnp.exp(scores - top), 0.0)
        self_weight = jnp.exp(self_score - top)
        total = jnp.sum(weights, axis=1, keepdims=True) + self_weight
        summed = jnp.dot(weights.astype(jnp.bfloat16), values, preferred_element_type=jnp.float32)
        summed = summed + self_weight.astype(jnp.bfloat16).astype(jnp.float32) * tiled_value
        attended = summed / total
        for g in range(GROUP):
            at = (k * GROUP + g) * HEAD_DIM
            out_ref[:, at : at + HEAD_DIM] = attended[g * count : (g + 1) * count].astype(
                jnp.bfloat16
            )


def attend_kernel(
    lengths_ref, place_ref, parts_ref, bias_ref, frequency_ref, cache_ref, stream_ref,
    out_ref, same_ref, *, width,
):
    same_ref[...] = stream_ref[...]
    attend_body(
        lengths_ref, place_ref, parts_ref, bias_ref, frequency_ref, cache_ref, out_ref, width
    )


def attend(lengths, place, parts, bias, frequency, cache, stream, width):
    count = parts.shape[1]
    return pl.pallas_call(
        functools.partial(attend_kernel, width=width),
        in_specs=[SMEM, SMEM] + [VMEM] * 5,
        out_specs=[VMEM] * 2,
        out_shape=[
            jax.ShapeDtypeStruct((count, HEADS * HEAD_DIM), jnp.bfloat16),
            jax.ShapeDtypeStruct(stream.shape, stream.dtype),
        ],
        compiler_params=PARAMS,
        cost_estimate=pl.CostEstimate(
            flops=COVER * stream.size * HEADS * HEAD_DIM, bytes_accessed=cache.size * 2, transcendentals=0
        ),
        name="attend",
    )(lengths, place, parts, bias, frequency, in_vmem(cache), stream)


def combine_kernel(gathered_ref, weight_ref, stream_ref, out_ref):
    peers = gathered_ref.shape[0]
    blocks = [gathered_ref[j].astype(jnp.float32) for j in range(peers)]
    gathered = jnp.concatenate(blocks, axis=0).astype(jnp.bfloat16)
    for at in range(0, out_ref.shape[1], OUT_CHUNK):
        update = jnp.dot(
            gathered, weight_ref[:, at : at + OUT_CHUNK], preferred_element_type=jnp.float32
        )
        current = stream_ref[:, at : at + OUT_CHUNK].astype(jnp.float32)
        out_ref[:, at : at + OUT_CHUNK] = (current + update).astype(jnp.bfloat16)


def combine(gathered, weight, stream):
    return pl.pallas_call(
        combine_kernel,
        in_specs=[VMEM, VMEM, VMEM],
        out_specs=VMEM,
        out_shape=jax.ShapeDtypeStruct(stream.shape, jnp.bfloat16),
        compiler_params=PARAMS,
        name="combine",
    )(gathered, in_vmem(weight), stream)


def total_square(ref):
    pieces, requests, _ = ref.shape
    squares = jnp.zeros((requests, 1), jnp.float32)
    for m in range(pieces):
        current = ref[m].astype(jnp.float32)
        squares = squares + jnp.sum(current * current, axis=1, keepdims=True)
    return squares


def square_kernel(rows_ref, out_ref):
    out_ref[...] = total_square(rows_ref)


def row_squares(rows):
    return pl.pallas_call(
        square_kernel,
        in_specs=[VMEM],
        out_specs=VMEM,
        out_shape=jax.ShapeDtypeStruct((rows.shape[1], 1), jnp.float32),
        compiler_params=PARAMS,
        cost_estimate=pl.CostEstimate(
            flops=COVER * rows.size * HEADS * LANES // 8, bytes_accessed=rows.size, transcendentals=0
        ),
        name="row_squares",
    )(rows)


def logits_kernel(
    assign_ref, tokens_ref, place_ref, rows_ref, over_ref, own_ref, gain_ref, weight_ref,
    logits_ref, stats_ref, scratch_ref, inverse_ref, *, width,
):
    pieces, requests, share = rows_ref.shape
    vocab = weight_ref.shape[1]
    own = place_ref[2] == 1
    inverse_ref[...] = lax.rsqrt(own_ref[...] / width + EPS)

    @pl.when(place_ref[2] != 1)
    def _():
        inverse_ref[...] = lax.rsqrt(total_square(over_ref) / width + EPS)

    inverse = inverse_ref[...]
    logits = jnp.zeros((requests, vocab), jnp.float32)
    for m in range(pieces):
        current = jnp.where(own, rows_ref[m], over_ref[m]).astype(jnp.float32)
        normed = (current * gain_ref[m].astype(jnp.float32) * inverse).astype(jnp.bfloat16)
        weight = weight_ref[m * share : (m + 1) * share]
        logits = logits + jnp.dot(normed, weight, preferred_element_type=jnp.float32)
    scratch_ref[...] = logits
    row = lax.broadcasted_iota(jnp.int32, (requests, vocab), 0)
    targets = jnp.zeros((requests, vocab), jnp.int32)
    for s in range(requests):
        request = assign_ref[s]
        logits_ref[pl.ds(s, 1), :] = scratch_ref[pl.ds(request, 1), :]
        targets = jnp.where(row == s, tokens_ref[request] - place_ref[1], targets)
    ordered = logits_ref[...]
    column = lax.broadcasted_iota(jnp.int32, (requests, vocab), 1)
    picked = jnp.sum(jnp.where(column == targets, ordered, 0.0), axis=1, keepdims=True)
    top = jnp.max(ordered, axis=1, keepdims=True)
    total = jnp.sum(jnp.exp(ordered - top), axis=1, keepdims=True)
    wide = (requests, stats_ref.shape[1])
    lane = lax.broadcasted_iota(jnp.int32, wide, 1) - lax.broadcasted_iota(jnp.int32, wide, 0)
    spread_out = jnp.where(lane == 0, top, 0.0)
    spread_out = jnp.where(lane == requests, total, spread_out)
    spread_out = jnp.where(lane == 2 * requests, picked, spread_out)
    stats_ref[...] = jnp.sum(spread_out, axis=0, keepdims=True)


def final_logits(assign, tokens, place, rows, over, own, gain, weight, width):
    requests = rows.shape[1]
    vocab = weight.shape[1]
    lanes = -(-3 * requests // LANES) * LANES
    return pl.pallas_call(
        functools.partial(logits_kernel, width=width),
        in_specs=[SMEM] * 3 + [VMEM] * 5,
        out_specs=[VMEM, VMEM],
        out_shape=[
            jax.ShapeDtypeStruct((requests, vocab), jnp.float32),
            jax.ShapeDtypeStruct((1, lanes), jnp.float32),
        ],
        scratch_shapes=[
            pltpu.VMEM((requests, vocab), jnp.float32),
            pltpu.VMEM((requests, 1), jnp.float32),
        ],
        compiler_params=PARAMS,
        name="final_logits",
    )(assign, tokens, place, rows, over, own, gain, in_vmem(weight))


def finish_kernel(logits_ref, stats_ref, out_ref, chosen_ref):
    requests = logits_ref.shape[0]
    stats = stats_ref[...]
    lanes = stats.shape[1]
    top = jnp.max(stats, axis=0, keepdims=True)
    sums = pltpu.roll(stats, lanes - requests, 1)
    picks = pltpu.roll(stats, lanes - 2 * requests, 1)
    total = jnp.sum(sums * jnp.exp(jnp.minimum(stats - top, 0.0)), axis=0, keepdims=True)
    lane = lax.broadcasted_iota(jnp.int32, (1, lanes), 1)
    total = jnp.where(lane < requests, total, 1.0)
    log_total = jnp.where(lane < requests, top, 0.0) + jnp.log(total)
    chosen_ref[...] = (jnp.sum(picks, axis=0, keepdims=True) - log_total)[:, :requests]
    wide = (requests, lanes)
    here = lax.broadcasted_iota(jnp.int32, wide, 1) == lax.broadcasted_iota(jnp.int32, wide, 0)
    column = jnp.sum(jnp.where(here, log_total, 0.0), axis=1, keepdims=True)
    out_ref[...] = logits_ref[...] - column


def finish(logits, stats):
    requests = logits.shape[0]
    return pl.pallas_call(
        finish_kernel,
        in_specs=[VMEM, VMEM],
        out_specs=[VMEM, VMEM],
        out_shape=[
            jax.ShapeDtypeStruct(logits.shape, jnp.float32),
            jax.ShapeDtypeStruct((1, requests), jnp.float32),
        ],
        compiler_params=PARAMS,
        name="finish",
    )(logits, stats)


def exchange(blocks, axis):
    return lax.all_to_all(blocks, axis, 0, 0, tiled=True)


def spread(value, axis):
    blocks = jnp.broadcast_to(value[None], (lax.axis_size(axis),) + value.shape)
    return exchange(blocks, axis)


def local(
    hidden_in,
    lengths,
    assign,
    token_ids,
    attn_gain,
    qkv_weight,
    qkv_bias,
    out_weight,
    kv_cache,
    final_gain,
    head_weight,
):
    sections = lax.axis_size("pipe")
    section = lax.axis_index("pipe")
    peers = lax.axis_size("mp")
    share = hidden_in.shape[1]
    width = share * peers
    vocab_first = lax.axis_index(("pipe", "mp")) * head_weight.shape[1]
    odd = section % 2 == 1
    place = jnp.stack([lax.axis_index("mp"), vocab_first, odd.astype(vocab_first.dtype)])
    place = place.astype(jnp.int32)
    exponents = np.arange(HEAD_DIM // 2, dtype=np.float64) * 2.0 / HEAD_DIM
    frequency = np.tile(THETA ** (-exponents), 2)[None, :].astype(np.float32)
    weight_in = qkv_weight[0]
    weight_out = out_weight[0]
    cache = kv_cache[0]
    final_row = final_gain[None]

    def layer_step(payload, current, cache_here, weight_here, bias_here):
        parts = exchange(payload, "mp")
        attended, current = attend(
            lengths, place, parts, bias_here, frequency, cache_here, current, width
        )
        return combine(spread(attended, "mp"), weight_here, current)

    def run_one(payload, current, gains, cache_ready):
        return layer_step(payload, current, cache_ready, weight_out, qkv_bias), gains

    def run_two(payload, current, gains, cache_ready, out_moved, bias_moved):
        current = layer_step(payload, current, cache_ready, out_moved, bias_moved)
        payload, cache_own = project_load(current, attn_gain, weight_in, cache, peers)
        return layer_step(payload, current, cache_own, weight_out, qkv_bias), gains

    def share_gains(payload, current, gains, *ready):
        return current, spread(final_row, "mp")

    def skip(payload, current, gains, *ready):
        return current, gains

    def move(array):
        return lax.ppermute(array, "pipe", [(i, i + 1) for i in range(2, sections, 2)])

    gain_full = jnp.zeros((peers, 1, share), final_gain.dtype)
    small = move(jnp.concatenate([attn_gain, qkv_bias], axis=1))
    in_moved, cache_moved, out_moved = move(weight_in), move(cache), move(weight_out)

    payload, stream, cache_ready = project_first(
        place, hidden_in, attn_gain, weight_in, cache, peers
    )
    stream, gain_full = lax.switch(
        jnp.where(section == 0, 0, 1), (run_one, share_gains), payload, stream, gain_full,
        cache_ready,
    )
    in_ready, cache_ready = load(0, stream, [weight_in, cache])
    stream = lax.ppermute(stream, "pipe", [(0, 1)])

    payload = project(stream, attn_gain, in_ready, peers)
    stream, gain_full = lax.switch(
        jnp.where(section == 1, 1, jnp.where(section == 0, 2, 0)),
        (skip, run_one, share_gains), payload, stream, gain_full, cache_ready,
    )
    for top in range(3, sections, 2):
        in_ready, cache_ready = load(top, stream, [in_moved, cache_moved])
        out_here = relay(out_moved)
        stream = lax.ppermute(stream, "pipe", [(top - 2, top)])
        payload = project(stream, small, in_ready, peers)
        stream, gain_full = lax.switch(
            (section == top).astype(jnp.int32),
            (skip, run_two), payload, stream, gain_full, cache_ready, out_here, small,
        )

    last = sections - 1
    arrived = stream
    for target in range(1, last, 2):
        copied = lax.ppermute(stream, "pipe", [(last, target)])
        arrived = jnp.where(section == target, copied, arrived)
    rows = lax.cond(
        odd,
        lambda b: spread(b, "mp"),
        lambda b: jnp.broadcast_to(b[None], (peers,) + b.shape),
        arrived,
    )
    over = lax.ppermute(rows, "pipe", [(i, i - 1) for i in range(1, sections, 2)])

    logits, stats = final_logits(
        assign, token_ids, place, rows, over, row_squares(rows), gain_full, head_weight, width
    )
    stats = spread(stats, ("pipe", "mp"))
    logprobs, chosen = finish(logits, stats.reshape(stats.shape[0], stats.shape[2]))
    return logprobs, chosen[0]


def solution(mesh):
    return jax.shard_map(
        local,
        mesh=mesh,
        in_specs=(
            P(None, "mp"),
            P(),
            P(),
            P(),
            P("pipe", "mp"),
            P("pipe", "mp", None),
            P("pipe", None),
            P("pipe", None, "mp"),
            P("pipe", "mp", None, None, None, None),
            P("mp"),
            P(None, ("pipe", "mp")),
        ),
        out_specs=(P(None, ("pipe", "mp")), P()),
        check_vma=False,
    )
```

```python
import functools

import jax
import jax.numpy as jnp
import numpy as np
from jax import lax
from jax.experimental import pallas as pl
from jax.experimental.pallas import tpu as pltpu
from jax.sharding import PartitionSpec as P


HEADS = 32
KV_HEADS = 4
HEAD_DIM = 128
GROUP = HEADS // KV_HEADS
EPS = 1e-06
THETA = 1000000.0
LANES = 128
CHUNK = 512
OUT_CHUNK = 256
COVER = 128
RELAY_PIECES = 4
GRANT = 10 * 1024 * 1024
FULL_GRANT = 60 * 1024 * 1024

VMEM = pl.BlockSpec(memory_space=pltpu.VMEM)
SMEM = pl.BlockSpec(memory_space=pltpu.SMEM)
HBM = pl.BlockSpec(memory_space=pltpu.HBM)
PARAMS = pltpu.CompilerParams(vmem_limit_bytes=GRANT)


def in_hbm(array):
    return pltpu.with_memory_space_constraint(array, pltpu.HBM)


def in_vmem(array):
    return pltpu.with_memory_space_constraint(array, pltpu.VMEM)


def column_copies(source, target, sem):
    return [
        pltpu.make_async_copy(
            source.at[:, pl.ds(i * CHUNK, CHUNK)], target.at[:, pl.ds(i * CHUNK, CHUNK)], sem.at[i]
        )
        for i in range(target.shape[1] // CHUNK)
    ]


def project_body(stream_ref, gain_ref, weight, out_ref, copies):
    peers, count, _ = out_ref.shape
    current = stream_ref[...].astype(jnp.float32)
    squares = jnp.sum(current * current, axis=1, keepdims=True)
    scaled = (current * gain_ref[:, : stream_ref.shape[1]].astype(jnp.float32)).astype(jnp.bfloat16)
    high = squares.astype(jnp.bfloat16).astype(jnp.float32)
    middle = (squares - high).astype(jnp.bfloat16).astype(jnp.float32)
    low = squares - high - middle
    lane = lax.broadcasted_iota(jnp.int32, (current.shape[0], LANES), 1)
    tail = jnp.where(lane == 0, high, jnp.where(lane == 1, middle, jnp.where(lane == 2, low, 0.0)))

    def store(block, at):
        for j in range(peers):
            out_ref[j, :, at : at + block.shape[1]] = block[j * count : (j + 1) * count].astype(
                jnp.bfloat16
            )

    store(tail, weight.shape[1])
    for i in range(weight.shape[1] // CHUNK):
        if copies is not None:
            copies[i].wait()
        block = jnp.dot(
            scaled,
            weight[:, i * CHUNK : (i + 1) * CHUNK],
            preferred_element_type=jnp.float32,
        )
        store(block, i * CHUNK)


def project_first_kernel(
    place_ref, stream_hbm, gain_hbm, source_ref, cache_hbm,
    out_ref, stream_ref, cache_ref, gain_ref, weight_ref, sem,
):
    del place_ref
    columns = weight_ref.shape[1] // CHUNK
    copy_stream = pltpu.make_async_copy(stream_hbm, stream_ref, sem.at[columns])
    copy_gain = pltpu.make_async_copy(gain_hbm, gain_ref, sem.at[columns + 1])
    copies = column_copies(source_ref, weight_ref, sem)
    copy_stream.start()
    copy_gain.start()
    for copy in copies:
        copy.start()
    copy_cache = pltpu.make_async_copy(cache_hbm, cache_ref, sem.at[columns + 2])
    copy_cache.start()
    copy_stream.wait()
    copy_gain.wait()
    project_body(stream_ref, gain_ref, weight_ref, out_ref, copies)
    copy_cache.wait()


def project_kernel(stream_ref, gain_ref, weight_ref, out_ref):
    project_body(stream_ref, gain_ref, weight_ref, out_ref, None)


def project_first(place, stream, gain, weight, cache, peers):
    columns = weight.shape[1]
    count = stream.shape[0] // peers
    return pl.pallas_call(
        project_first_kernel,
        in_specs=[SMEM] + [HBM] * 4,
        out_specs=[VMEM] * 3,
        out_shape=[
            jax.ShapeDtypeStruct((peers, count, columns + LANES), jnp.bfloat16),
            pltpu.VMEM(stream.shape, stream.dtype),
            pltpu.VMEM(cache.shape, cache.dtype),
        ],
        scratch_shapes=[
            pltpu.VMEM(gain.shape, gain.dtype),
            pltpu.VMEM(weight.shape, weight.dtype),
            pltpu.SemaphoreType.DMA((columns // CHUNK + 3,)),
        ],
        compiler_params=pltpu.CompilerParams(vmem_limit_bytes=FULL_GRANT),
        name="project_first",
    )(place, in_hbm(stream), in_hbm(gain), in_hbm(weight), in_hbm(cache))


def load_kernel(order_ref, after_ref, *refs):
    del order_ref, after_ref
    count = len(refs) // 2
    sem = refs[-1]
    copies = [
        pltpu.make_async_copy(
            refs[i].at[pl.ds(0, refs[count + i].shape[0])], refs[count + i], sem.at[i]
        )
        for i in range(count)
    ]
    for copy in copies:
        copy.start()
    for copy in copies:
        copy.wait()


def load(order, after, arrays, rows=None):
    shapes = [array.shape if rows is None else (rows,) + array.shape[1:] for array in arrays]
    size = sum(array.size for array in arrays)
    return pl.pallas_call(
        load_kernel,
        in_specs=[SMEM, VMEM] + [HBM] * len(arrays),
        out_specs=[VMEM] * len(arrays),
        out_shape=[pltpu.VMEM(shape, array.dtype) for shape, array in zip(shapes, arrays)],
        scratch_shapes=[pltpu.SemaphoreType.DMA((len(arrays),))],
        compiler_params=PARAMS,
        cost_estimate=pl.CostEstimate(flops=4 * size, bytes_accessed=4 * size, transcendentals=0),
        name="load",
    )(jnp.full((1,), order, jnp.int32), after, *[in_hbm(array) for array in arrays])


def relay_kernel(source_ref, out_ref, buffer_ref, sem_in, sem_out):
    pieces = sem_in.shape[0]
    size = source_ref.shape[0] // pieces
    spans = [pl.ds(i * size, size) for i in range(pieces)]
    arrive = [
        pltpu.make_async_copy(source_ref.at[span], buffer_ref.at[span], sem_in.at[i])
        for i, span in enumerate(spans)
    ]
    leave = [
        pltpu.make_async_copy(buffer_ref.at[span], out_ref.at[span], sem_out.at[i])
        for i, span in enumerate(spans)
    ]
    for copy in arrive:
        copy.start()
    for i in range(pieces):
        arrive[i].wait()
        leave[i].start()
    for copy in leave:
        copy.wait()


def relay(array):
    return pl.pallas_call(
        relay_kernel,
        in_specs=[HBM],
        out_specs=pl.BlockSpec(memory_space=pl.ANY),
        out_shape=jax.ShapeDtypeStruct(array.shape, array.dtype),
        scratch_shapes=[
            pltpu.VMEM(array.shape, array.dtype),
            pltpu.SemaphoreType.DMA((RELAY_PIECES,)),
            pltpu.SemaphoreType.DMA((RELAY_PIECES,)),
        ],
        compiler_params=PARAMS,
        cost_estimate=pl.CostEstimate(
            flops=4 * array.size, bytes_accessed=4 * array.size, transcendentals=0
        ),
        name="relay",
    )(in_hbm(array))


def project(stream, gain, weight, peers):
    columns = weight.shape[1]
    count = stream.shape[0] // peers
    return pl.pallas_call(
        project_kernel,
        in_specs=[VMEM, VMEM, VMEM],
        out_specs=VMEM,
        out_shape=jax.ShapeDtypeStruct((peers, count, columns + LANES), jnp.bfloat16),
        compiler_params=PARAMS,
        name="project",
    )(stream, gain, in_vmem(weight))


def project_load_kernel(stream_ref, gain_ref, weight_ref, cache_hbm, out_ref, cache_ref, sem):
    copy = pltpu.make_async_copy(cache_hbm, cache_ref, sem.at[0])
    copy.start()
    project_body(stream_ref, gain_ref, weight_ref, out_ref, None)
    copy.wait()


def project_load(stream, gain, weight, cache, peers):
    columns = weight.shape[1]
    count = stream.shape[0] // peers
    return pl.pallas_call(
        project_load_kernel,
        in_specs=[VMEM, VMEM, VMEM, HBM],
        out_specs=[VMEM, VMEM],
        out_shape=[
            jax.ShapeDtypeStruct((peers, count, columns + LANES), jnp.bfloat16),
            pltpu.VMEM(cache.shape, cache.dtype),
        ],
        scratch_shapes=[pltpu.SemaphoreType.DMA((1,))],
        compiler_params=PARAMS,
        name="project_load",
    )(stream, gain, in_vmem(weight), in_hbm(cache))


def attend_body(lengths_ref, place_ref, parts_ref, bias_ref, frequency_ref, cache, out_ref, width):
    count = out_ref.shape[0]
    length = cache.shape[3]
    query_cols = HEADS * HEAD_DIM
    key_cols = KV_HEADS * HEAD_DIM
    first = place_ref[0] * count
    at_row = lax.broadcasted_iota(jnp.int32, (count, HEAD_DIM), 0)
    positions = jnp.zeros((count, HEAD_DIM), jnp.int32)
    wide = (GROUP * count, count * length)
    at_wide = lax.broadcasted_iota(jnp.int32, (GROUP * count, 1), 0) % count
    limit = jnp.zeros((GROUP * count, 1), jnp.int32)
    for r in range(count):
        position = lengths_ref[first + r]
        positions = jnp.where(at_row == r, position, positions)
        limit = jnp.where(at_wide == r, position, limit)
    offset = lax.broadcasted_iota(jnp.int32, wide, 1) - at_wide * length
    visible = (offset >= 0) & (offset < limit)
    angles = positions.astype(jnp.float32) * frequency_ref[...]
    lane = lax.broadcasted_iota(jnp.int32, (count, HEAD_DIM), 1)
    cosine = jnp.cos(angles)
    sine = jnp.sin(angles)
    sine = jnp.where(lane < HEAD_DIM // 2, -sine, sine)

    def total_of(at, size):
        acc = parts_ref[0, :, at : at + size].astype(jnp.float32)
        for j in range(1, parts_ref.shape[0]):
            acc = acc + parts_ref[j, :, at : at + size].astype(jnp.float32)
        return acc

    squares = jnp.sum(total_of(query_cols + 2 * key_cols, LANES), axis=1, keepdims=True)
    inverse = lax.rsqrt(squares / width + EPS)

    def columns_of(at):
        shifted = at + bias_ref.shape[1] - (query_cols + 2 * key_cols)
        bias = bias_ref[:, shifted : shifted + HEAD_DIM].astype(jnp.float32)
        return total_of(at, HEAD_DIM) * inverse + bias

    def rotate(head):
        return head * cosine + pltpu.roll(head, HEAD_DIM // 2, 1) * sine

    scale = HEAD_DIM ** (-0.5)
    heads = []
    for k in range(KV_HEADS):
        stack = [rotate(columns_of((k * GROUP + g) * HEAD_DIM)) for g in range(GROUP)]
        queries = jnp.concatenate(stack, axis=0).astype(jnp.bfloat16)
        key_new = rotate(columns_of(query_cols + k * HEAD_DIM))
        key_new = key_new.astype(jnp.bfloat16).astype(jnp.float32)
        value_new = columns_of(query_cols + key_cols + k * HEAD_DIM)
        value_new = value_new.astype(jnp.bfloat16).astype(jnp.float32)
        heads.append((queries, key_new, value_new))
    raw = []
    for k in range(KV_HEADS):
        keys = cache[:, 0, k].reshape(count * length, HEAD_DIM)
        raw.append(
            lax.dot_general(
                heads[k][0], keys, (((1,), (1,)), ((), ())), preferred_element_type=jnp.float32
            )
        )
    mixed = []
    for k in range(KV_HEADS):
        queries, key_new, value_new = heads[k]
        tiled_key = jnp.concatenate([key_new] * GROUP, axis=0)
        self_score = (
            jnp.sum(queries.astype(jnp.float32) * tiled_key, axis=1, keepdims=True) * scale
        )
        scores = jnp.where(visible, raw[k] * scale, -1e30)
        top = jnp.maximum(jnp.max(scores, axis=1, keepdims=True), self_score)
        weights = jnp.exp(scores - top)
        self_weight = jnp.exp(self_score - top)
        total = jnp.sum(weights, axis=1, keepdims=True) + self_weight
        mixed.append((weights.astype(jnp.bfloat16), self_weight, total))
    for k in range(KV_HEADS):
        weights, self_weight, total = mixed[k]
        values = cache[:, 1, k].reshape(count * length, HEAD_DIM)
        tiled_value = jnp.concatenate([heads[k][2]] * GROUP, axis=0)
        summed = jnp.dot(weights, values, preferred_element_type=jnp.float32)
        summed = summed + self_weight.astype(jnp.bfloat16).astype(jnp.float32) * tiled_value
        attended = summed / total
        for g in range(GROUP):
            at = (k * GROUP + g) * HEAD_DIM
            out_ref[:, at : at + HEAD_DIM] = attended[g * count : (g + 1) * count].astype(
                jnp.bfloat16
            )


def attend_kernel(
    lengths_ref, place_ref, parts_ref, bias_ref, frequency_ref, cache_ref, stream_ref,
    out_ref, same_ref, *, width,
):
    same_ref[...] = stream_ref[...]
    attend_body(
        lengths_ref, place_ref, parts_ref, bias_ref, frequency_ref, cache_ref, out_ref, width
    )


def attend(lengths, place, parts, bias, frequency, cache, stream, width):
    count = parts.shape[1]
    return pl.pallas_call(
        functools.partial(attend_kernel, width=width),
        in_specs=[SMEM, SMEM] + [VMEM] * 5,
        out_specs=[VMEM] * 2,
        out_shape=[
            jax.ShapeDtypeStruct((count, HEADS * HEAD_DIM), jnp.bfloat16),
            jax.ShapeDtypeStruct(stream.shape, stream.dtype),
        ],
        compiler_params=PARAMS,
        cost_estimate=pl.CostEstimate(
            flops=COVER * stream.size * HEADS * HEAD_DIM, bytes_accessed=cache.size * 2, transcendentals=0
        ),
        name="attend",
    )(lengths, place, parts, bias, frequency, in_vmem(cache), stream)


def combine_kernel(gathered_ref, weight_ref, stream_ref, out_ref):
    peers = gathered_ref.shape[0]
    blocks = [gathered_ref[j].astype(jnp.float32) for j in range(peers)]
    gathered = jnp.concatenate(blocks, axis=0).astype(jnp.bfloat16)
    for at in range(0, out_ref.shape[1], OUT_CHUNK):
        update = jnp.dot(
            gathered, weight_ref[:, at : at + OUT_CHUNK], preferred_element_type=jnp.float32
        )
        current = stream_ref[:, at : at + OUT_CHUNK].astype(jnp.float32)
        out_ref[:, at : at + OUT_CHUNK] = (current + update).astype(jnp.bfloat16)


def combine(gathered, weight, stream):
    return pl.pallas_call(
        combine_kernel,
        in_specs=[VMEM, VMEM, VMEM],
        out_specs=VMEM,
        out_shape=jax.ShapeDtypeStruct(stream.shape, jnp.bfloat16),
        compiler_params=PARAMS,
        name="combine",
    )(gathered, in_vmem(weight), stream)


def total_square(ref):
    pieces, requests, _ = ref.shape
    squares = jnp.zeros((requests, 1), jnp.float32)
    for m in range(pieces):
        current = ref[m].astype(jnp.float32)
        squares = squares + jnp.sum(current * current, axis=1, keepdims=True)
    return squares


def square_kernel(rows_ref, out_ref):
    out_ref[...] = total_square(rows_ref)


def row_squares(rows):
    return pl.pallas_call(
        square_kernel,
        in_specs=[VMEM],
        out_specs=VMEM,
        out_shape=jax.ShapeDtypeStruct((rows.shape[1], 1), jnp.float32),
        compiler_params=PARAMS,
        cost_estimate=pl.CostEstimate(
            flops=COVER * rows.size * HEADS * LANES // 8, bytes_accessed=rows.size, transcendentals=0
        ),
        name="row_squares",
    )(rows)


def logits_kernel(
    assign_ref, tokens_ref, place_ref, rows_ref, over_ref, own_ref, gain_ref, weight_ref,
    logits_ref, stats_ref, scratch_ref, inverse_ref, *, width,
):
    pieces, requests, share = rows_ref.shape
    vocab = weight_ref.shape[1]
    own = place_ref[2] == 1
    inverse_ref[...] = lax.rsqrt(own_ref[...] / width + EPS)

    @pl.when(place_ref[2] != 1)
    def _():
        inverse_ref[...] = lax.rsqrt(total_square(over_ref) / width + EPS)

    inverse = inverse_ref[...]
    logits = jnp.zeros((requests, vocab), jnp.float32)
    for m in range(pieces):
        current = jnp.where(own, rows_ref[m], over_ref[m]).astype(jnp.float32)
        normed = (current * gain_ref[m].astype(jnp.float32) * inverse).astype(jnp.bfloat16)
        weight = weight_ref[m * share : (m + 1) * share]
        logits = logits + jnp.dot(normed, weight, preferred_element_type=jnp.float32)
    scratch_ref[...] = logits
    row = lax.broadcasted_iota(jnp.int32, (requests, vocab), 0)
    targets = jnp.zeros((requests, vocab), jnp.int32)
    for s in range(requests):
        request = assign_ref[s]
        logits_ref[pl.ds(s, 1), :] = scratch_ref[pl.ds(request, 1), :]
        targets = jnp.where(row == s, tokens_ref[request] - place_ref[1], targets)
    ordered = logits_ref[...]
    column = lax.broadcasted_iota(jnp.int32, (requests, vocab), 1)
    picked = jnp.sum(jnp.where(column == targets, ordered, 0.0), axis=1, keepdims=True)
    top = jnp.max(ordered, axis=1, keepdims=True)
    total = jnp.sum(jnp.exp(ordered - top), axis=1, keepdims=True)
    wide = (requests, stats_ref.shape[1])
    lane = lax.broadcasted_iota(jnp.int32, wide, 1) - lax.broadcasted_iota(jnp.int32, wide, 0)
    spread_out = jnp.where(lane == 0, top, 0.0)
    spread_out = jnp.where(lane == requests, total, spread_out)
    spread_out = jnp.where(lane == 2 * requests, picked, spread_out)
    stats_ref[...] = jnp.sum(spread_out, axis=0, keepdims=True)


def final_logits(assign, tokens, place, rows, over, own, gain, weight, width):
    requests = rows.shape[1]
    vocab = weight.shape[1]
    lanes = -(-3 * requests // LANES) * LANES
    return pl.pallas_call(
        functools.partial(logits_kernel, width=width),
        in_specs=[SMEM] * 3 + [VMEM] * 5,
        out_specs=[VMEM, VMEM],
        out_shape=[
            jax.ShapeDtypeStruct((requests, vocab), jnp.float32),
            jax.ShapeDtypeStruct((1, lanes), jnp.float32),
        ],
        scratch_shapes=[
            pltpu.VMEM((requests, vocab), jnp.float32),
            pltpu.VMEM((requests, 1), jnp.float32),
        ],
        compiler_params=PARAMS,
        name="final_logits",
    )(assign, tokens, place, rows, over, own, gain, in_vmem(weight))


def finish_kernel(logits_ref, stats_ref, out_ref, chosen_ref):
    requests = logits_ref.shape[0]
    stats = stats_ref[...]
    lanes = stats.shape[1]
    top = jnp.max(stats, axis=0, keepdims=True)
    sums = pltpu.roll(stats, lanes - requests, 1)
    picks = pltpu.roll(stats, lanes - 2 * requests, 1)
    total = jnp.sum(sums * jnp.exp(jnp.minimum(stats - top, 0.0)), axis=0, keepdims=True)
    lane = lax.broadcasted_iota(jnp.int32, (1, lanes), 1)
    total = jnp.where(lane < requests, total, 1.0)
    log_total = jnp.where(lane < requests, top, 0.0) + jnp.log(total)
    chosen_ref[...] = (jnp.sum(picks, axis=0, keepdims=True) - log_total)[:, :requests]
    wide = (requests, lanes)
    here = lax.broadcasted_iota(jnp.int32, wide, 1) == lax.broadcasted_iota(jnp.int32, wide, 0)
    column = jnp.sum(jnp.where(here, log_total, 0.0), axis=1, keepdims=True)
    out_ref[...] = logits_ref[...] - column


def finish(logits, stats):
    requests = logits.shape[0]
    return pl.pallas_call(
        finish_kernel,
        in_specs=[VMEM, VMEM],
        out_specs=[VMEM, VMEM],
        out_shape=[
            jax.ShapeDtypeStruct(logits.shape, jnp.float32),
            jax.ShapeDtypeStruct((1, requests), jnp.float32),
        ],
        compiler_params=PARAMS,
        name="finish",
    )(logits, stats)


def exchange(blocks, axis):
    return lax.all_to_all(blocks, axis, 0, 0, tiled=True)


def spread(value, axis):
    blocks = jnp.broadcast_to(value[None], (lax.axis_size(axis),) + value.shape)
    return exchange(blocks, axis)


def local(
    hidden_in,
    lengths,
    assign,
    token_ids,
    attn_gain,
    qkv_weight,
    qkv_bias,
    out_weight,
    kv_cache,
    final_gain,
    head_weight,
):
    sections = lax.axis_size("pipe")
    section = lax.axis_index("pipe")
    peers = lax.axis_size("mp")
    share = hidden_in.shape[1]
    width = share * peers
    vocab_first = lax.axis_index(("pipe", "mp")) * head_weight.shape[1]
    odd = section % 2 == 1
    place = jnp.stack([lax.axis_index("mp"), vocab_first, odd.astype(vocab_first.dtype)])
    place = place.astype(jnp.int32)
    exponents = np.arange(HEAD_DIM // 2, dtype=np.float64) * 2.0 / HEAD_DIM
    frequency = np.tile(THETA ** (-exponents), 2)[None, :].astype(np.float32)
    weight_in = qkv_weight[0]
    weight_out = out_weight[0]
    cache = kv_cache[0]
    final_row = final_gain[None]

    def layer_step(payload, current, cache_here, weight_here, bias_here):
        parts = exchange(payload, "mp")
        attended, current = attend(
            lengths, place, parts, bias_here, frequency, cache_here, current, width
        )
        return combine(spread(attended, "mp"), weight_here, current)

    def run_one(payload, current, gains, cache_ready):
        return layer_step(payload, current, cache_ready, weight_out, qkv_bias), gains

    def run_two(payload, current, gains, cache_ready, out_moved, bias_moved):
        current = layer_step(payload, current, cache_ready, out_moved, bias_moved)
        payload, cache_own = project_load(current, attn_gain, weight_in, cache, peers)
        return layer_step(payload, current, cache_own, weight_out, qkv_bias), gains

    def share_gains(payload, current, gains, *ready):
        return current, spread(final_row, "mp")

    def skip(payload, current, gains, *ready):
        return current, gains

    def move(array):
        return lax.ppermute(array, "pipe", [(i, i + 1) for i in range(2, sections, 2)])

    gain_full = jnp.zeros((peers, 1, share), final_gain.dtype)
    small = move(jnp.concatenate([attn_gain, qkv_bias], axis=1))
    in_moved, cache_moved, out_moved = move(weight_in), move(cache), move(weight_out)

    payload, stream, cache_ready = project_first(
        place, hidden_in, attn_gain, weight_in, cache, peers
    )
    stream, gain_full = lax.switch(
        jnp.where(section == 0, 0, 1), (run_one, share_gains), payload, stream, gain_full,
        cache_ready,
    )
    in_ready, cache_ready = load(0, stream, [weight_in, cache])
    stream = lax.ppermute(stream, "pipe", [(0, 1)])

    payload = project(stream, attn_gain, in_ready, peers)
    stream, gain_full = lax.switch(
        jnp.where(section == 1, 1, jnp.where(section == 0, 2, 0)),
        (skip, run_one, share_gains), payload, stream, gain_full, cache_ready,
    )
    for top in range(3, sections, 2):
        in_ready, cache_ready = load(top, stream, [in_moved, cache_moved])
        out_here = relay(out_moved)
        stream = lax.ppermute(stream, "pipe", [(top - 2, top)])
        payload = project(stream, small, in_ready, peers)
        stream, gain_full = lax.switch(
            (section == top).astype(jnp.int32),
            (skip, run_two), payload, stream, gain_full, cache_ready, out_here, small,
        )

    last = sections - 1
    arrived = stream
    for target in range(1, last, 2):
        copied = lax.ppermute(stream, "pipe", [(last, target)])
        arrived = jnp.where(section == target, copied, arrived)
    rows = lax.cond(
        odd,
        lambda b: spread(b, "mp"),
        lambda b: jnp.broadcast_to(b[None], (peers,) + b.shape),
        arrived,
    )
    over = lax.ppermute(rows, "pipe", [(i, i - 1) for i in range(1, sections, 2)])

    logits, stats = final_logits(
        assign, token_ids, place, rows, over, row_squares(rows), gain_full, head_weight, width
    )
    stats = spread(stats, ("pipe", "mp"))
    logprobs, chosen = finish(logits, stats.reshape(stats.shape[0], stats.shape[2]))
    return logprobs, chosen[0]


def solution(mesh):
    return jax.shard_map(
        local,
        mesh=mesh,
        in_specs=(
            P(None, "mp"),
            P(),
            P(),
            P(),
            P("pipe", "mp"),
            P("pipe", "mp", None),
            P("pipe", None),
            P("pipe", None, "mp"),
            P("pipe", "mp", None, None, None, None),
            P("mp"),
            P(None, ("pipe", "mp")),
        ),
        out_specs=(P(None, ("pipe", "mp")), P()),
        check_vma=False,
    )
```
